32 devices in a mesh: tm: 8 (over z, y), series: 4 (over x, core).
Axes of the slice: x: 2, y: 2, z: 4, core: 2. Of those that a mesh axis runs over, the one named last changes fastest.
Arguments:
- signal: float32 [64, 262144], P('series', 'tm')
- valid_start: int32 [64], replicated, may hold values from 0 to 65535
- valid_end: int32 [64], replicated, may hold values from 196609 to 262144
Outputs:
- smooth: float32 [64, 262144], P('series', 'tm')
- slope: float32 [64, 262144], P('series', 'tm')
- covariance: float32 [64, 64], P('series')
The draws below stay inside these ranges and needn't reach their ends.
Inputs may be any that keep to these rules, and one draw needn't show every extreme that they name: `valid_end`: end of the valid samples of each series.
All inputs are finite; a program needn't handle non-finite values.
Results may differ from the reference program's by a relative error of at most 0.00015.
Values sent between devices are 32-bit elements; how exact they have to be, the bound alone decides.
A program may use at most 64 MiB of HBM per device.

```python
import math
import jax
import jax.numpy as jnp
from jax import lax

HALF = 16
S = 64
NT = 262144


def draw_signal(key, part):
    keys = jax.random.split(jax.random.fold_in(key, 17), 6)
    times = jnp.arange(NT).astype(jnp.float32) / NT
    rising = 0.5 + times
    mixing = jax.random.uniform(keys[0], (S, 1), jnp.float32, -1.0, 1.0)
    phase = jax.random.uniform(keys[4], (S, 1), jnp.float32, 0.0, 2.0 * math.pi)
    freq = jax.random.uniform(keys[5], (S, 1), jnp.float32, 3.0, 9.0)
    trend = jnp.sin(2.0 * math.pi * freq * times[None, :] + phase)
    common = jax.random.normal(keys[1], (NT,), jnp.float32)
    own = jax.random.normal(keys[2], (S, NT), jnp.float32)
    noise = 0.8 * rising[None, :] * (mixing * common[None, :] + own)
    return trend + noise


def set_ends(array, key, smallest, largest):
    dims = array.shape
    place = [jax.random.randint(jax.random.fold_in(key, axis), (), 0, dims[axis]) for axis in range(len(dims))]
    array = array.at[tuple(place)].set(smallest)
    longest = dims.index(max(dims))
    place[longest] = (place[longest] + 1) % dims[longest]
    return array.at[tuple(place)].set(largest)


def setup_inputs(seed: int = 0) -> dict:
    seeds = jax.random.split(jax.random.key(seed), 4)
    return {
        "signal": draw_signal(jax.random.fold_in(seeds[3], 71), 0),
        "valid_start": set_ends(jax.random.randint(seeds[1], (S,), 0, NT // 4), jax.random.fold_in(seeds[1], 1), 0, (NT // 4) - 1).astype(jnp.int32),
        "valid_end": set_ends(jax.random.randint(seeds[2], (S,), NT - NT // 4 + 1, NT + 1), jax.random.fold_in(seeds[2], 1), NT - NT // 4 + 1, NT).astype(jnp.int32),
    }


def reference(signal, valid_start, valid_end):
    taps = 2 * HALF + 1
    offsets = jnp.arange(-HALF, HALF + 1).astype(jnp.float32)
    second = jnp.sum(offsets * offsets)
    centre_sq = second / taps
    curved = offsets * offsets - centre_sq
    fourth = jnp.sum(curved * curved)
    padded = jnp.pad(signal, ((0, 0), (HALF, HALF)))
    level = jnp.zeros_like(signal)
    tilt = jnp.zeros_like(signal)
    bend = jnp.zeros_like(signal)
    for m in range(taps):
        window = padded[:, m:m + NT]
        level = level + window * (1.0 / taps)
        tilt = tilt + window * (offsets[m] / second)
        bend = bend + window * (curved[m] / fourth)
    first = valid_start.astype(jnp.int32)[:, None]
    last = valid_end.astype(jnp.int32)[:, None]
    moment = jnp.arange(NT, dtype=jnp.int32)[None, :]
    centre = jnp.clip(moment, first + HALF, last - HALF - 1).astype(jnp.int32)
    along = (moment - centre).astype(jnp.float32)
    lv = jnp.take_along_axis(level, centre, axis=1)
    tl = jnp.take_along_axis(tilt, centre, axis=1)
    bd = jnp.take_along_axis(bend, centre, axis=1)
    inside = (moment >= first) & (moment < last)
    smooth = jnp.where(inside, lv + tl * along + bd * (along * along - centre_sq), 0.0)
    slope = jnp.where(inside, HALF * (tl + 2.0 * along * bd), 0.0)
    resid = jnp.where(inside, signal - smooth, 0.0)
    gram = lax.dot_general(resid, resid, (((1,), (1,)), ((), ())), precision=lax.Precision.HIGHEST, preferred_element_type=jnp.float32)
    correlation = (jnp.minimum(last, valid_end[None, :]) - jnp.maximum(first, valid_start[None, :])).astype(jnp.float32)
    return smooth, slope, gram / correlation
```

```python
import functools

import jax
import jax.numpy as jnp
from jax import lax
from jax.experimental import pallas as pl
from jax.experimental.pallas import tpu as pltpu
from jax.sharding import PartitionSpec as P

HALF = 16
LANE = 128
TAPS = 2 * HALF + 1
SECOND = float(sum(j * j for j in range(-HALF, HALF + 1)))
CENTRE_SQ = SECOND / TAPS
FOURTH = float(sum((j * j - CENTRE_SQ) ** 2 for j in range(-HALF, HALF + 1)))
MESH = pl.DeviceIdType.MESH


def chunk_of(quarter):
    chunk = 1024
    while quarter % chunk:
        chunk //= 2
    return chunk


def kernel(
    n_s, n_t, rows, width, chunk,
    start_hbm, end_hbm, sig_hbm,
    smooth, slope, cov,
    starts, stops, ext, wts, ends, res, mixed, halo, part, r1, mine, r2,
    load_sem, bound_sem, halo_send, halo_recv, send_sem, recv_sem, s1_sem, s2_sem, met,
):
    s = lax.axis_index("series")
    t = lax.axis_index("tm")
    quarter = width // n_s
    per = quarter // chunk
    steps = n_s * per
    sends = (n_s - 1) * per
    total = n_s * rows
    tiles = chunk // LANE
    group = 2 - n_t % 2
    f32 = jnp.float32

    def offset(qi):
        if n_s == 4:
            odd = lax.rem(s, 2)
            return jnp.where(qi == 0, 2, jnp.where(qi == 1, 3 - 2 * odd, jnp.where(qi == 2, 1 + 2 * odd, 0)))
        return lax.rem(qi + 1, n_s)

    def fetch(at, size, sem):
        return pltpu.make_async_copy(
            sig_hbm.at[:, pl.ds(pl.multiple_of(at, LANE), size)],
            ext.at[:, pl.ds(pl.multiple_of(at + LANE, LANE), size)],
            load_sem.at[sem])

    head = lax.rem(s + offset(0), n_s) * quarter
    lead = min(chunk + 2 * LANE, quarter - chunk + LANE)
    before = chunk - LANE
    after = quarter - before - lead
    fetch(head + before, lead, 0).start()

    partner = t + 1 - 2 * lax.rem(t, 2)

    def tell(sem, at, ok=None):
        def signal():
            pl.semaphore_signal(sem, inc=1, device_id={"tm": at}, device_id_type=MESH)
        if ok is None:
            signal()
        else:
            pl.when(ok)(signal)

    def reach(sem, far):
        tell(sem, t - far, t >= far)
        tell(sem, t + far, t + far < n_t)

    def heard(far):
        return (t >= far).astype(jnp.int32) + (t + far < n_t).astype(jnp.int32)

    barrier = pltpu.get_barrier_semaphore()
    for d in range(1, n_s):
        pl.semaphore_signal(barrier, inc=1, device_id={"series": lax.rem(s + d, n_s)}, device_id_type=MESH)
    if group == 2:
        tell(barrier, partner)
    reach(barrier, group)

    limits = [
        pltpu.make_async_copy(start_hbm, starts, bound_sem.at[0]),
        pltpu.make_async_copy(end_hbm, stops, bound_sem.at[1]),
    ]
    for limit in limits:
        limit.start()
    fetch(head, before, 1).start()
    if after:
        fetch(head + before + lead, after, 1).start()
    for qi in range(1, n_s):
        fetch(lax.rem(s + offset(qi), n_s) * quarter, quarter, 1).start()

    tap = lax.broadcasted_iota(jnp.int32, (2 * LANE, LANE), 0) - lax.broadcasted_iota(jnp.int32, (2 * LANE, LANE), 1) - HALF
    near = (tap >= -HALF) & (tap <= HALF)
    tap = tap.astype(f32)
    wts[:, :LANE] = jnp.where(near, 1.0 / TAPS - (tap * tap - CENTRE_SQ) * (CENTRE_SQ / FOURTH), 0.0)
    wts[:, LANE:] = jnp.where(near, tap * (HALF / SECOND), 0.0)
    ext[:, :LANE] = jnp.zeros((rows, LANE), f32)
    ext[:, LANE + width :] = jnp.zeros((rows, LANE), f32)

    for limit in limits:
        limit.wait()
    row = lax.broadcasted_iota(jnp.int32, (rows, LANE), 0)
    begin = t * width
    first = jnp.zeros((rows, LANE), jnp.int32)
    last = jnp.zeros((rows, LANE), jnp.int32)
    for i in range(rows):
        first = jnp.where(row == i, starts[s * rows + i], first)
        last = jnp.where(row == i, stops[s * rows + i], last)
    ends[0] = first - begin
    ends[1] = last - begin

    def held(v, base):
        lanes = lax.broadcasted_iota(jnp.int32, (rows, LANE), 1)
        found = []
        for spot in (ends[0] + LANE - base, ends[1] - TAPS + LANE - base):
            tile = lax.shift_right_arithmetic(spot, LANE.bit_length() - 1)
            pair = [jnp.zeros((rows, LANE), f32)] * 2
            for n in range(tiles + 1):
                here = tile == n
                for w in range(2):
                    pair[w] = jnp.where(here, v[:, (n + w) * LANE : (n + w + 1) * LANE], pair[w])
            j = lanes - (spot - tile * LANE + HALF)
            sums = []
            for j, win in ((j, pair[0]), (j + LANE, pair[1])):
                win = jnp.where((j >= -HALF) & (j <= HALF), win, 0.0)
                j = j.astype(f32)
                sums.append((win, win * j, win * (j * j - CENTRE_SQ)))
            for m, scale in enumerate((1.0 / TAPS, 1.0 / SECOND, 1.0 / FOURTH)):
                value = jnp.sum(sums[0][m] + sums[1][m], axis=1, keepdims=True) * scale
                found.append(jnp.broadcast_to(value, (rows, LANE)))
        return found

    right, left = lax.rem(t + 1, n_t), lax.rem(t + n_t - 1, n_t)
    to_right = pltpu.make_async_remote_copy(
        ext.at[:, pl.ds(width, LANE)], halo.at[0], halo_send.at[0], halo_recv.at[0],
        device_id={"tm": right}, device_id_type=MESH)
    to_left = pltpu.make_async_remote_copy(
        ext.at[:, pl.ds(LANE, LANE)], halo.at[1], halo_send.at[1], halo_recv.at[1],
        device_id={"tm": left}, device_id_type=MESH)
    has_right, has_left = t < n_t - 1, t > 0

    def place(k):
        qi = k // per
        q = lax.rem(s + offset(qi), n_s)
        j = lax.rem(lax.rem(k, per) + 1, per)
        return q, j

    def transfer(k):
        q, j = place(k)
        return pltpu.make_async_remote_copy(
            res.at[:, pl.ds(pl.multiple_of(q * quarter + j * chunk, chunk), chunk)],
            mixed.at[s, :, pl.ds(pl.multiple_of(j * chunk, chunk), chunk)],
            send_sem, recv_sem.at[j],
            device_id={"series": q}, device_id_type=MESH)

    def spread(v):
        return jnp.concatenate([v] * tiles, axis=1)

    greet = min(3, per - 3)

    def step(k, carry):
        @pl.when(k == 0)
        def _():
            fetch(0, lead, 0).wait()

        @pl.when(k == 1)
        def _():
            fetch(0, width - lead, 1).wait()

        @pl.when(k == per - 2)
        def _():
            @pl.when(has_left)
            def _():
                to_right.wait_recv()
                ext[:, :LANE] = halo[0]

            @pl.when(has_right)
            def _():
                to_left.wait_recv()
                ext[:, LANE + width :] = halo[1]

        q, j = place(k)
        base = pl.multiple_of(q * quarter + j * chunk, chunk)
        v = ext[:, pl.ds(base, chunk + 2 * LANE)]
        moved = pltpu.roll(v, chunk + LANE + HALF, 1)
        lines = jnp.concatenate([moved[:, n * LANE : (n + 2) * LANE] for n in range(tiles)], axis=0)
        out = jnp.dot(lines, wts[...], precision=lax.Precision.HIGHEST, preferred_element_type=f32)
        sm = jnp.concatenate([out[n * rows : (n + 1) * rows, :LANE] for n in range(tiles)], axis=1)
        sl = jnp.concatenate([out[n * rows : (n + 1) * rows, LANE:] for n in range(tiles)], axis=1)
        moment = base + lax.broadcasted_iota(jnp.int32, (rows, chunk), 1)
        low = moment - spread(ends[0])
        high = moment - spread(ends[1])
        coef = held(v, base)
        inside = (low >= 0) & (high < 0)
        below = low < HALF
        above = high >= -HALF
        along = jnp.where(below, low - HALF, high + HALF + 1).astype(f32)
        lv = jnp.where(below, spread(coef[0]), spread(coef[3]))
        tl = jnp.where(below, spread(coef[1]), spread(coef[4]))
        bd = jnp.where(below, spread(coef[2]), spread(coef[5]))
        end = below | above
        sm = jnp.where(end, lv + tl * along + bd * (along * along - CENTRE_SQ), sm)
        sl = jnp.where(end, HALF * (tl + 2.0 * along * bd), sl)
        sm = jnp.where(inside, sm, 0.0)
        smooth[:, pl.ds(base, chunk)] = sm
        slope[:, pl.ds(base, chunk)] = jnp.where(inside, sl, 0.0)
        rs = jnp.where(inside, v[:, LANE : LANE + chunk] - sm, 0.0)

        @pl.when(k < sends)
        def _():
            res[:, pl.ds(base, chunk)] = rs

        @pl.when(k >= sends)
        def _():
            mixed[s, :, pl.ds(pl.multiple_of(j * chunk, chunk), chunk)] = rs

        @pl.when(k == 0)
        def _():
            pl.semaphore_wait(barrier, n_s - 1 + group - 1 + heard(group))
            if group == 2:
                tell(met.at[0], partner)
            reach(met.at[0], group)

        @pl.when(k == greet)
        def _():
            pl.semaphore_wait(met.at[0], group - 1 + heard(group))

            @pl.when(has_right)
            def _():
                to_right.start()

            @pl.when(has_left)
            def _():
                to_left.start()

        @pl.when((k >= 1) & (k <= sends))
        def _():
            transfer(k - 1).start()

        return carry

    lax.fori_loop(0, steps, step, 0)

    rounds = []
    far = 2 * group
    while far < n_t:
        rounds.append(far)
        far *= 2
    rounds.append(0)

    def greeting(i):
        if i > len(rounds):
            return
        if i > 0:
            far = rounds[i - 1]
            if far:
                pl.semaphore_wait(met.at[i], heard(far))
            elif group == 2:
                pl.semaphore_wait(met.at[i], 1)
        if i < len(rounds):
            far = rounds[i]
            if far:
                reach(met.at[i + 1], far)
            elif group == 2:
                tell(met.at[i + 1], partner)

    def arrival(i):
        j = (i + 1) % per
        block = mixed.at[pl.ds(0, n_s - 1), :, pl.ds(pl.multiple_of(j * chunk, chunk), chunk)]
        return pltpu.make_async_remote_copy(
            block, block, send_sem, recv_sem.at[j],
            device_id={"series": lax.rem(s + 1, n_s)}, device_id_type=MESH)

    half = rows // 2
    left_half = lax.broadcasted_iota(jnp.int32, (half, 2 * total), 1) < total

    def pack(v):
        return jnp.where(left_half, v[:half], v[half:])

    gram = jnp.zeros((2 * total, 2 * total), f32)
    for i in range(per):
        greeting(i)
        arrival(i).wait_recv()
        j = (i + 1) % per
        x = jnp.concatenate(
            [mixed[g, :, pl.ds(pl.multiple_of(j * chunk, chunk), chunk)] for g in range(n_s)], axis=0)
        hi = x.astype(jnp.bfloat16)
        lo = (x - hi.astype(f32)).astype(jnp.bfloat16)
        z = jnp.concatenate([hi, lo], axis=0)
        gram = gram + lax.dot_general(z, z, (((1,), (1,)), ((), ())), preferred_element_type=f32)
    for i in range(per, len(rounds) + 1):
        greeting(i)
    both = gram[:total] + gram[total:]
    both = both + pltpu.roll(both, total, 1)
    for g in range(n_s):
        part[g] = pack(both[g * rows : (g + 1) * rows])

    def first_stage(d):
        peer = lax.rem(s + d, n_s)
        return pltpu.make_async_remote_copy(
            part.at[peer], r1.at[d - 1], s1_sem.at[0], s1_sem.at[1],
            device_id={"series": peer}, device_id_type=MESH)

    for d in range(1, n_s):
        first_stage(d).start()

    lane = lax.broadcasted_iota(jnp.int32, (rows, 2 * total), 1)
    lane = jnp.where(lane < total, lane, lane - total)
    first_k = jnp.zeros((rows, 2 * total), jnp.int32)
    last_k = jnp.zeros((rows, 2 * total), jnp.int32)
    for i in range(total):
        first_k = jnp.where(lane == i, starts[i], first_k)
        last_k = jnp.where(lane == i, stops[i], last_k)
    count = pack((jnp.minimum(last_k, last) - jnp.maximum(first_k, first)).astype(f32))

    def gather(ref, sems):
        return pltpu.make_async_remote_copy(
            ref, ref, sems.at[0], sems.at[1], device_id={"series": lax.rem(s + 1, n_s)}, device_id_type=MESH)

    own = part[s]
    gather(r1, s1_sem).wait_recv()
    for d in range(1, n_s):
        own = own + r1[d - 1]
    mine[...] = own

    def second_stage(d):
        return pltpu.make_async_remote_copy(
            mine, r2.at[t], s2_sem.at[0], s2_sem.at[1],
            device_id={"tm": lax.rem(t + d, n_t)}, device_id_type=MESH)

    for d in range(1, n_t):
        second_stage(d).start()
    r2[t] = own
    sent = res.at[:, pl.ds(0, sends * chunk)]
    pltpu.make_async_remote_copy(
        sent, sent, send_sem, recv_sem.at[0],
        device_id={"series": lax.rem(s + 1, n_s)}, device_id_type=MESH).wait_send()

    @pl.when(has_right)
    def _():
        to_right.wait_send()

    @pl.when(has_left)
    def _():
        to_left.wait_send()

    gather(r1, s1_sem).wait_send()
    gather(r2.at[pl.ds(0, n_t - 1)], s2_sem).wait_recv()
    full = r2[0]
    for d in range(1, n_t):
        full = full + r2[d]
    full = full / count
    cov[:half] = full[:, :total]
    cov[half:] = pltpu.roll(full, total, 1)[:, :total]
    gather(r2.at[pl.ds(0, n_t - 1)], s2_sem).wait_send()


FLUSHES = 4


def flush(smooth, slope, cov, smooth_out, slope_out, cov_out, sems, cov_sem):
    piece = smooth.shape[1] // FLUSHES
    copies = [pltpu.make_async_copy(cov, cov_out, cov_sem)]
    for i in range(FLUSHES):
        span = pl.ds(i * piece, piece)
        copies.append(pltpu.make_async_copy(smooth.at[:, span], smooth_out.at[:, span], sems.at[2 * i]))
        copies.append(pltpu.make_async_copy(slope.at[:, span], slope_out.at[:, span], sems.at[2 * i + 1]))
    for copy in copies:
        copy.start()
    for copy in copies:
        copy.wait()


def solution(mesh):
    n_t, n_s = mesh.shape["tm"], mesh.shape["series"]

    def shards(signal, valid_start, valid_end):
        rows, width = signal.shape
        total = rows * n_s
        quarter = width // n_s
        chunk = chunk_of(quarter)
        per = quarter // chunk
        f32 = jnp.float32
        dma = pltpu.SemaphoreType.DMA
        kept = pl.pallas_call(
            functools.partial(kernel, n_s, n_t, rows, width, chunk),
            out_shape=(
                jax.ShapeDtypeStruct((rows, width), f32),
                jax.ShapeDtypeStruct((rows, width), f32),
                jax.ShapeDtypeStruct((rows, total), f32),
            ),
            in_specs=[pl.BlockSpec(memory_space=pltpu.HBM)] * 3,
            out_specs=(pl.BlockSpec(memory_space=pltpu.VMEM),) * 3,
            scratch_shapes=[
                pltpu.SMEM((total,), jnp.int32),
                pltpu.SMEM((total,), jnp.int32),
                pltpu.VMEM((rows, width + 2 * LANE), f32),
                pltpu.VMEM((2 * LANE, 2 * LANE), f32),
                pltpu.VMEM((2, rows, LANE), jnp.int32),
                pltpu.VMEM((rows, width), f32),
                pltpu.VMEM((n_s, rows, quarter), f32),
                pltpu.VMEM((2, rows, LANE), f32),
                pltpu.VMEM((n_s, rows // 2, 2 * total), f32),
                pltpu.VMEM((n_s - 1, rows // 2, 2 * total), f32),
                pltpu.VMEM((rows // 2, 2 * total), f32),
                pltpu.VMEM((n_t, rows // 2, 2 * total), f32),
                dma((2,)),
                dma((2,)),
                dma((2,)),
                dma((2,)),
                dma,
                dma((per,)),
                dma((2,)),
                dma((2,)),
                pltpu.SemaphoreType.REGULAR((n_t.bit_length() + 1,)),
            ],
            compiler_params=pltpu.CompilerParams(
                collective_id=0, has_side_effects=True, vmem_limit_bytes=67043328 - 8 * rows * width - 12 * 1024 * 1024
            ),
        )(valid_start, valid_end, signal)
        return pl.pallas_call(
            flush,
            out_shape=tuple(jax.ShapeDtypeStruct(v.shape, f32) for v in kept),
            in_specs=[pl.BlockSpec(memory_space=pltpu.VMEM)] * 3,
            out_specs=(pl.BlockSpec(memory_space=pltpu.HBM),) * 3,
            scratch_shapes=[dma((2 * FLUSHES,)), dma],
            compiler_params=pltpu.CompilerParams(vmem_limit_bytes=1024 * 1024),
        )(*kept)

    in_specs = (P("series", "tm"), P(), P())
    out_specs = (P("series", "tm"), P("series", "tm"), P("series", None))
    return jax.shard_map(shards, mesh=mesh, in_specs=in_specs, out_specs=out_specs, check_vma=False)
```

```python
import functools

import jax
import jax.numpy as jnp
from jax import lax
from jax.experimental import pallas as pl
from jax.experimental.pallas import tpu as pltpu
from jax.sharding import PartitionSpec as P

HALF = 16
LANE = 128
TAPS = 2 * HALF + 1
SECOND = float(sum(j * j for j in range(-HALF, HALF + 1)))
CENTRE_SQ = SECOND / TAPS
FOURTH = float(sum((j * j - CENTRE_SQ) ** 2 for j in range(-HALF, HALF + 1)))
MESH = pl.DeviceIdType.MESH


def chunk_of(quarter):
    chunk = 1024
    while quarter % chunk:
        chunk //= 2
    return chunk


def kernel(
    n_s, n_t, rows, width, chunk,
    start_hbm, end_hbm, sig_hbm,
    smooth, slope, cov,
    starts, stops, ext, wts, ends, res, mixed, halo, part, shares,
    load_sem, bound_sem, halo_send, halo_recv, send_sem, recv_sem, share_sem, met,
):
    s = lax.axis_index("series")
    t = lax.axis_index("tm")
    quarter = width // n_s
    per = quarter // chunk
    steps = n_s * per
    sends = (n_s - 1) * per
    total = n_s * rows
    tiles = chunk // LANE
    group = 2 - n_t % 2
    f32 = jnp.float32

    def offset(qi):
        if n_s == 4:
            odd = lax.rem(s, 2)
            return jnp.where(qi == 0, 2, jnp.where(qi == 1, 3 - 2 * odd, jnp.where(qi == 2, 1 + 2 * odd, 0)))
        return lax.rem(qi + 1, n_s)

    def fetch(at, size, sem):
        return pltpu.make_async_copy(
            sig_hbm.at[:, pl.ds(pl.multiple_of(at, LANE), size)],
            ext.at[:, pl.ds(pl.multiple_of(at + LANE, LANE), size)],
            load_sem.at[sem])

    head = lax.rem(s + offset(0), n_s) * quarter
    lead = min(chunk + 2 * LANE, quarter - chunk + LANE)
    before = chunk - LANE
    after = quarter - before - lead
    fetch(head + before, lead, 0).start()

    partner = t + 1 - 2 * lax.rem(t, 2)

    def tell(sem, at, ok=None):
        def signal():
            pl.semaphore_signal(sem, inc=1, device_id={"tm": at}, device_id_type=MESH)
        if ok is None:
            signal()
        else:
            pl.when(ok)(signal)

    def reach(sem, far):
        tell(sem, t - far, t >= far)
        tell(sem, t + far, t + far < n_t)

    def heard(far):
        return (t >= far).astype(jnp.int32) + (t + far < n_t).astype(jnp.int32)

    barrier = pltpu.get_barrier_semaphore()
    for d in range(1, n_s):
        pl.semaphore_signal(barrier, inc=1, device_id={"series": lax.rem(s + d, n_s)}, device_id_type=MESH)
    if group == 2:
        tell(barrier, partner)
    reach(barrier, group)

    limits = [
        pltpu.make_async_copy(start_hbm, starts, bound_sem.at[0]),
        pltpu.make_async_copy(end_hbm, stops, bound_sem.at[1]),
    ]
    for limit in limits:
        limit.start()
    fetch(head, before, 1).start()
    if after:
        fetch(head + before + lead, after, 1).start()
    for qi in range(1, n_s):
        fetch(lax.rem(s + offset(qi), n_s) * quarter, quarter, 1).start()

    tap = lax.broadcasted_iota(jnp.int32, (2 * LANE, LANE), 0) - lax.broadcasted_iota(jnp.int32, (2 * LANE, LANE), 1) - HALF
    near = (tap >= -HALF) & (tap <= HALF)
    tap = tap.astype(f32)
    wts[:, :LANE] = jnp.where(near, 1.0 / TAPS - (tap * tap - CENTRE_SQ) * (CENTRE_SQ / FOURTH), 0.0)
    wts[:, LANE:] = jnp.where(near, tap * (HALF / SECOND), 0.0)
    ext[:, :LANE] = jnp.zeros((rows, LANE), f32)
    ext[:, LANE + width :] = jnp.zeros((rows, LANE), f32)

    for limit in limits:
        limit.wait()
    row = lax.broadcasted_iota(jnp.int32, (rows, LANE), 0)
    begin = t * width
    first = jnp.zeros((rows, LANE), jnp.int32)
    last = jnp.zeros((rows, LANE), jnp.int32)
    for i in range(rows):
        first = jnp.where(row == i, starts[s * rows + i], first)
        last = jnp.where(row == i, stops[s * rows + i], last)
    ends[0] = first - begin
    ends[1] = last - begin

    def held(v, base):
        lanes = lax.broadcasted_iota(jnp.int32, (rows, LANE), 1)
        found = []
        for spot in (ends[0] + LANE - base, ends[1] - TAPS + LANE - base):
            tile = lax.shift_right_arithmetic(spot, LANE.bit_length() - 1)
            pair = [jnp.zeros((rows, LANE), f32)] * 2
            for n in range(tiles + 1):
                here = tile == n
                for w in range(2):
                    pair[w] = jnp.where(here, v[:, (n + w) * LANE : (n + w + 1) * LANE], pair[w])
            j = lanes - (spot - tile * LANE + HALF)
            sums = []
            for j, win in ((j, pair[0]), (j + LANE, pair[1])):
                win = jnp.where((j >= -HALF) & (j <= HALF), win, 0.0)
                j = j.astype(f32)
                sums.append((win, win * j, win * (j * j - CENTRE_SQ)))
            for m, scale in enumerate((1.0 / TAPS, 1.0 / SECOND, 1.0 / FOURTH)):
                value = jnp.sum(sums[0][m] + sums[1][m], axis=1, keepdims=True) * scale
                found.append(jnp.broadcast_to(value, (rows, LANE)))
        return found

    right, left = lax.rem(t + 1, n_t), lax.rem(t + n_t - 1, n_t)
    to_right = pltpu.make_async_remote_copy(
        ext.at[:, pl.ds(width, LANE)], halo.at[0], halo_send.at[0], halo_recv.at[0],
        device_id={"tm": right}, device_id_type=MESH)
    to_left = pltpu.make_async_remote_copy(
        ext.at[:, pl.ds(LANE, LANE)], halo.at[1], halo_send.at[1], halo_recv.at[1],
        device_id={"tm": left}, device_id_type=MESH)
    has_right, has_left = t < n_t - 1, t > 0

    def place(k):
        qi = k // per
        q = lax.rem(s + offset(qi), n_s)
        j = lax.rem(lax.rem(k, per) + 1, per)
        return q, j

    def transfer(k):
        q, j = place(k)
        return pltpu.make_async_remote_copy(
            res.at[:, pl.ds(pl.multiple_of(q * quarter + j * chunk, chunk), chunk)],
            mixed.at[s, :, pl.ds(pl.multiple_of(j * chunk, chunk), chunk)],
            send_sem, recv_sem.at[j],
            device_id={"series": q}, device_id_type=MESH)

    def spread(v):
        return jnp.concatenate([v] * tiles, axis=1)

    greet = min(3, per - 3)

    def step(k, carry):
        @pl.when(k == 0)
        def _():
            fetch(0, lead, 0).wait()

        @pl.when(k == 1)
        def _():
            fetch(0, width - lead, 1).wait()

        @pl.when(k == per - 2)
        def _():
            @pl.when(has_left)
            def _():
                to_right.wait_recv()
                ext[:, :LANE] = halo[0]

            @pl.when(has_right)
            def _():
                to_left.wait_recv()
                ext[:, LANE + width :] = halo[1]

        q, j = place(k)
        base = pl.multiple_of(q * quarter + j * chunk, chunk)
        v = ext[:, pl.ds(base, chunk + 2 * LANE)]
        moved = pltpu.roll(v, chunk + LANE + HALF, 1)
        lines = jnp.concatenate([moved[:, n * LANE : (n + 2) * LANE] for n in range(tiles)], axis=0)
        out = jnp.dot(lines, wts[...], precision=lax.Precision.HIGHEST, preferred_element_type=f32)
        sm = jnp.concatenate([out[n * rows : (n + 1) * rows, :LANE] for n in range(tiles)], axis=1)
        sl = jnp.concatenate([out[n * rows : (n + 1) * rows, LANE:] for n in range(tiles)], axis=1)
        moment = base + lax.broadcasted_iota(jnp.int32, (rows, chunk), 1)
        low = moment - spread(ends[0])
        high = moment - spread(ends[1])
        coef = held(v, base)
        inside = (low >= 0) & (high < 0)
        below = low < HALF
        above = high >= -HALF
        along = jnp.where(below, low - HALF, high + HALF + 1).astype(f32)
        lv = jnp.where(below, spread(coef[0]), spread(coef[3]))
        tl = jnp.where(below, spread(coef[1]), spread(coef[4]))
        bd = jnp.where(below, spread(coef[2]), spread(coef[5]))
        end = below | above
        sm = jnp.where(end, lv + tl * along + bd * (along * along - CENTRE_SQ), sm)
        sl = jnp.where(end, HALF * (tl + 2.0 * along * bd), sl)
        sm = jnp.where(inside, sm, 0.0)
        smooth[:, pl.ds(base, chunk)] = sm
        slope[:, pl.ds(base, chunk)] = jnp.where(inside, sl, 0.0)
        rs = jnp.where(inside, v[:, LANE : LANE + chunk] - sm, 0.0)

        @pl.when(k < sends)
        def _():
            res[:, pl.ds(base, chunk)] = rs

        @pl.when(k >= sends)
        def _():
            mixed[s, :, pl.ds(pl.multiple_of(j * chunk, chunk), chunk)] = rs

        @pl.when(k == 0)
        def _():
            pl.semaphore_wait(barrier, n_s - 1 + group - 1 + heard(group))
            if group == 2:
                tell(met.at[0], partner)
            reach(met.at[0], group)

        @pl.when(k == greet)
        def _():
            pl.semaphore_wait(met.at[0], group - 1 + heard(group))

            @pl.when(has_right)
            def _():
                to_right.start()

            @pl.when(has_left)
            def _():
                to_left.start()

        @pl.when((k >= 1) & (k <= sends))
        def _():
            transfer(k - 1).start()

        return carry

    lax.fori_loop(0, steps, step, 0)

    rounds = []
    far = 2 * group
    while far < n_t:
        rounds.append(far)
        far *= 2
    rounds.append(0)

    def greeting(i):
        if i > len(rounds):
            return
        if i > 0:
            far = rounds[i - 1]
            if far:
                pl.semaphore_wait(met.at[i], heard(far))
            elif group == 2:
                pl.semaphore_wait(met.at[i], 1)
        if i < len(rounds):
            far = rounds[i]
            if far:
                reach(met.at[i + 1], far)
            elif group == 2:
                tell(met.at[i + 1], partner)

    def arrival(i):
        j = (i + 1) % per
        block = mixed.at[pl.ds(0, n_s - 1), :, pl.ds(pl.multiple_of(j * chunk, chunk), chunk)]
        return pltpu.make_async_remote_copy(
            block, block, send_sem, recv_sem.at[j],
            device_id={"series": lax.rem(s + 1, n_s)}, device_id_type=MESH)

    half = rows // 2
    left_half = lax.broadcasted_iota(jnp.int32, (half, 2 * total), 1) < total

    def pack(v):
        return jnp.where(left_half, v[:half], v[half:])

    gram = jnp.zeros((2 * total, 2 * total), f32)
    for i in range(per):
        greeting(i)
        arrival(i).wait_recv()
        j = (i + 1) % per
        x = jnp.concatenate(
            [mixed[g, :, pl.ds(pl.multiple_of(j * chunk, chunk), chunk)] for g in range(n_s)], axis=0)
        hi = x.astype(jnp.bfloat16)
        lo = (x - hi.astype(f32)).astype(jnp.bfloat16)
        z = jnp.concatenate([hi, lo], axis=0)
        gram = gram + lax.dot_general(z, z, (((1,), (1,)), ((), ())), preferred_element_type=f32)
    for i in range(per, len(rounds) + 1):
        greeting(i)
    both = gram[:total] + gram[total:]
    both = both + pltpu.roll(both, total, 1)
    for g in range(n_s):
        part[g] = pack(both[g * rows : (g + 1) * rows])

    here = t * n_s + s
    peers = n_t * n_s - 1

    def share(i):
        peer = jnp.where(i < here, i, i + 1)
        to_t, to_s = lax.div(peer, n_s), lax.rem(peer, n_s)
        return pltpu.make_async_remote_copy(
            part.at[to_s], shares.at[here], share_sem.at[0], share_sem.at[1],
            device_id={"tm": to_t, "series": to_s}, device_id_type=MESH)

    def spread_shares(i, carry):
        share(i).start()
        return carry

    lax.fori_loop(0, peers, spread_shares, 0)
    shares[here] = part[s]

    lane = lax.broadcasted_iota(jnp.int32, (rows, 2 * total), 1)
    lane = jnp.where(lane < total, lane, lane - total)
    first_k = jnp.zeros((rows, 2 * total), jnp.int32)
    last_k = jnp.zeros((rows, 2 * total), jnp.int32)
    for i in range(total):
        first_k = jnp.where(lane == i, starts[i], first_k)
        last_k = jnp.where(lane == i, stops[i], last_k)
    count = pack((jnp.minimum(last_k, last) - jnp.maximum(first_k, first)).astype(f32))

    sent = res.at[:, pl.ds(0, sends * chunk)]
    pltpu.make_async_remote_copy(
        sent, sent, send_sem, recv_sem.at[0],
        device_id={"series": lax.rem(s + 1, n_s)}, device_id_type=MESH).wait_send()

    @pl.when(has_right)
    def _():
        to_right.wait_send()

    @pl.when(has_left)
    def _():
        to_left.wait_send()

    others = shares.at[pl.ds(0, peers)]
    shared = pltpu.make_async_remote_copy(
        others, others, share_sem.at[0], share_sem.at[1],
        device_id={"series": lax.rem(s + 1, n_s)}, device_id_type=MESH)
    shared.wait_recv()
    full = shares[0]
    for d in range(1, peers + 1):
        full = full + shares[d]
    full = full / count
    cov[:half] = full[:, :total]
    cov[half:] = pltpu.roll(full, total, 1)[:, :total]
    shared.wait_send()


FLUSHES = 4


def flush(smooth, slope, cov, smooth_out, slope_out, cov_out, sems, cov_sem):
    piece = smooth.shape[1] // FLUSHES
    copies = [pltpu.make_async_copy(cov, cov_out, cov_sem)]
    for i in range(FLUSHES):
        span = pl.ds(i * piece, piece)
        copies.append(pltpu.make_async_copy(smooth.at[:, span], smooth_out.at[:, span], sems.at[2 * i]))
        copies.append(pltpu.make_async_copy(slope.at[:, span], slope_out.at[:, span], sems.at[2 * i + 1]))
    for copy in copies:
        copy.start()
    for copy in copies:
        copy.wait()


def solution(mesh):
    n_t, n_s = mesh.shape["tm"], mesh.shape["series"]

    def shards(signal, valid_start, valid_end):
        rows, width = signal.shape
        total = rows * n_s
        quarter = width // n_s
        chunk = chunk_of(quarter)
        per = quarter // chunk
        f32 = jnp.float32
        dma = pltpu.SemaphoreType.DMA
        kept = pl.pallas_call(
            functools.partial(kernel, n_s, n_t, rows, width, chunk),
            out_shape=(
                jax.ShapeDtypeStruct((rows, width), f32),
                jax.ShapeDtypeStruct((rows, width), f32),
                jax.ShapeDtypeStruct((rows, total), f32),
            ),
            in_specs=[pl.BlockSpec(memory_space=pltpu.HBM)] * 3,
            out_specs=(pl.BlockSpec(memory_space=pltpu.VMEM),) * 3,
            scratch_shapes=[
                pltpu.SMEM((total,), jnp.int32),
                pltpu.SMEM((total,), jnp.int32),
                pltpu.VMEM((rows, width + 2 * LANE), f32),
                pltpu.VMEM((2 * LANE, 2 * LANE), f32),
                pltpu.VMEM((2, rows, LANE), jnp.int32),
                pltpu.VMEM((rows, width), f32),
                pltpu.VMEM((n_s, rows, quarter), f32),
                pltpu.VMEM((2, rows, LANE), f32),
                pltpu.VMEM((n_s, rows // 2, 2 * total), f32),
                pltpu.VMEM((n_t * n_s, rows // 2, 2 * total), f32),
                dma((2,)),
                dma((2,)),
                dma((2,)),
                dma((2,)),
                dma,
                dma((per,)),
                dma((2,)),
                pltpu.SemaphoreType.REGULAR((n_t.bit_length() + 1,)),
            ],
            compiler_params=pltpu.CompilerParams(
                collective_id=0, has_side_effects=True, vmem_limit_bytes=67043328 - 8 * rows * width - 12 * 1024 * 1024
            ),
        )(*[pltpu.with_memory_space_constraint(v, pltpu.HBM) for v in (valid_start, valid_end)], signal)
        return pl.pallas_call(
            flush,
            out_shape=tuple(jax.ShapeDtypeStruct(v.shape, f32) for v in kept),
            in_specs=[pl.BlockSpec(memory_space=pltpu.VMEM)] * 3,
            out_specs=(pl.BlockSpec(memory_space=pltpu.HBM),) * 3,
            scratch_shapes=[dma((2 * FLUSHES,)), dma],
            compiler_params=pltpu.CompilerParams(vmem_limit_bytes=1024 * 1024),
        )(*kept)

    in_specs = (P("series", "tm"), P(), P())
    out_specs = (P("series", "tm"), P("series", "tm"), P("series", None))
    return jax.shard_map(shards, mesh=mesh, in_specs=in_specs, out_specs=out_specs, check_vma=False)
```

```python
import functools

import jax
import jax.numpy as jnp
from jax import lax
from jax.experimental import pallas as pl
from jax.experimental.pallas import tpu as pltpu
from jax.sharding import PartitionSpec as P

HALF = 16
LANE = 128
TAPS = 2 * HALF + 1
SECOND = float(sum(j * j for j in range(-HALF, HALF + 1)))
CENTRE_SQ = SECOND / TAPS
FOURTH = float(sum((j * j - CENTRE_SQ) ** 2 for j in range(-HALF, HALF + 1)))
MESH = pl.DeviceIdType.MESH


def chunk_of(quarter):
    chunk = 1024
    while quarter % chunk:
        chunk //= 2
    return chunk


def kernel(
    n_s, n_t, rows, width, chunk,
    start_hbm, end_hbm, sig_hbm,
    smooth, slope, cov,
    starts, stops, ext, wts, ends, res, mixed, halo, part, shares, relay,
    load_sem, bound_sem, halo_send, halo_recv, send_sem, recv_sem, share_sem, met, relay_send, relay_recv,
):
    s = lax.axis_index("series")
    t = lax.axis_index("tm")
    quarter = width // n_s
    per = quarter // chunk
    steps = n_s * per
    sends = (n_s - 1) * per
    total = n_s * rows
    tiles = chunk // LANE
    group = 2 - n_t % 2
    pairs = n_t // group
    rounds = []
    far = 2 * group
    while far < n_t:
        rounds.append(far)
        far *= 2
    rounds.append(0)
    swaps = n_s == 4 and len(rounds) > 1 and per >= 8
    f32 = jnp.float32

    def offset(qi):
        if n_s == 4:
            odd = lax.rem(s, 2)
            return jnp.where(qi == 0, 2, jnp.where(qi == 1, 3 - 2 * odd, jnp.where(qi == 2, 1 + 2 * odd, 0)))
        return lax.rem(qi + 1, n_s)

    def fetch(at, size, sem):
        return pltpu.make_async_copy(
            sig_hbm.at[:, pl.ds(pl.multiple_of(at, LANE), size)],
            ext.at[:, pl.ds(pl.multiple_of(at + LANE, LANE), size)],
            load_sem.at[sem])

    head = lax.rem(s + offset(0), n_s) * quarter
    lead = min(chunk + 2 * LANE, quarter - chunk + LANE)
    before = chunk - LANE
    after = quarter - before - lead
    fetch(head + before, lead, 0).start()

    partner = t + 1 - 2 * lax.rem(t, 2)

    def tell(sem, at, ok=None):
        def signal():
            pl.semaphore_signal(sem, inc=1, device_id={"tm": at}, device_id_type=MESH)
        if ok is None:
            signal()
        else:
            pl.when(ok)(signal)

    def reach(sem, far):
        tell(sem, t - far, t >= far)
        tell(sem, t + far, t + far < n_t)

    def heard(far):
        return (t >= far).astype(jnp.int32) + (t + far < n_t).astype(jnp.int32)

    barrier = pltpu.get_barrier_semaphore()
    for d in range(1, n_s):
        pl.semaphore_signal(barrier, inc=1, device_id={"series": lax.rem(s + d, n_s)}, device_id_type=MESH)
    if group == 2:
        tell(barrier, partner)
    reach(barrier, group)

    limits = [
        pltpu.make_async_copy(start_hbm, starts, bound_sem.at[0]),
        pltpu.make_async_copy(end_hbm, stops, bound_sem.at[1]),
    ]
    for limit in limits:
        limit.start()
    fetch(head, before, 1).start()
    if after:
        fetch(head + before + lead, after, 1).start()
    for qi in range(1, n_s):
        fetch(lax.rem(s + offset(qi), n_s) * quarter, quarter, 1).start()

    tap = lax.broadcasted_iota(jnp.int32, (2 * LANE, LANE), 0) - lax.broadcasted_iota(jnp.int32, (2 * LANE, LANE), 1) - HALF
    near = (tap >= -HALF) & (tap <= HALF)
    tap = tap.astype(f32)
    wts[:, :LANE] = jnp.where(near, 1.0 / TAPS - (tap * tap - CENTRE_SQ) * (CENTRE_SQ / FOURTH), 0.0)
    wts[:, LANE:] = jnp.where(near, tap * (HALF / SECOND), 0.0)
    ext[:, :LANE] = jnp.zeros((rows, LANE), f32)
    ext[:, LANE + width :] = jnp.zeros((rows, LANE), f32)

    for limit in limits:
        limit.wait()
    row = lax.broadcasted_iota(jnp.int32, (rows, LANE), 0)
    begin = t * width
    first = jnp.zeros((rows, LANE), jnp.int32)
    last = jnp.zeros((rows, LANE), jnp.int32)
    for i in range(rows):
        first = jnp.where(row == i, starts[s * rows + i], first)
        last = jnp.where(row == i, stops[s * rows + i], last)
    ends[0] = first - begin
    ends[1] = last - begin

    def held(v, base):
        lanes = lax.broadcasted_iota(jnp.int32, (rows, LANE), 1)
        found = []
        for spot in (ends[0] + LANE - base, ends[1] - TAPS + LANE - base):
            tile = lax.shift_right_arithmetic(spot, LANE.bit_length() - 1)
            pair = [jnp.zeros((rows, LANE), f32)] * 2
            for n in range(tiles + 1):
                here = tile == n
                for w in range(2):
                    pair[w] = jnp.where(here, v[:, (n + w) * LANE : (n + w + 1) * LANE], pair[w])
            j = lanes - (spot - tile * LANE + HALF)
            sums = []
            for j, win in ((j, pair[0]), (j + LANE, pair[1])):
                win = jnp.where((j >= -HALF) & (j <= HALF), win, 0.0)
                j = j.astype(f32)
                sums.append((win, win * j, win * (j * j - CENTRE_SQ)))
            for m, scale in enumerate((1.0 / TAPS, 1.0 / SECOND, 1.0 / FOURTH)):
                value = jnp.sum(sums[0][m] + sums[1][m], axis=1, keepdims=True) * scale
                found.append(jnp.broadcast_to(value, (rows, LANE)))
        return found

    right, left = lax.rem(t + 1, n_t), lax.rem(t + n_t - 1, n_t)
    to_right = pltpu.make_async_remote_copy(
        ext.at[:, pl.ds(width, LANE)], halo.at[0], halo_send.at[0], halo_recv.at[0],
        device_id={"tm": right}, device_id_type=MESH)
    to_left = pltpu.make_async_remote_copy(
        ext.at[:, pl.ds(LANE, LANE)], halo.at[1], halo_send.at[1], halo_recv.at[1],
        device_id={"tm": left}, device_id_type=MESH)
    has_right, has_left = t < n_t - 1, t > 0

    mirror = t + group * (pairs - 1 - 2 * lax.div(t, group))
    gap = lax.div(t - mirror, group)
    whole_from, whole_to = gap == 3, gap == -3
    half_from, half_to = gap == 1, gap == -1
    detour = per + 2
    across = lax.rem(s + offset(1), n_s)

    def place(k):
        qi = k // per
        q = lax.rem(s + offset(qi), n_s)
        j = lax.rem(lax.rem(k, per) + 1, per)
        return q, j

    def transfer(k):
        q, j = place(k)
        return pltpu.make_async_remote_copy(
            res.at[:, pl.ds(pl.multiple_of(q * quarter + j * chunk, chunk), chunk)],
            mixed.at[s, :, pl.ds(pl.multiple_of(j * chunk, chunk), chunk)],
            send_sem, recv_sem.at[j],
            device_id={"series": q}, device_id_type=MESH)

    def column(j):
        return pl.multiple_of(j * chunk, chunk)

    def away(k, n):
        q, j = place(k)
        size = chunk if n == 0 else chunk // 2
        return pltpu.make_async_remote_copy(
            res.at[:, pl.ds(column(q * per + j), size)], relay.at[n, :, pl.ds(0, size)],
            send_sem, relay_recv.at[n],
            device_id={"series": across, "tm": mirror}, device_id_type=MESH)

    def onward(n):
        j = detour + n - per + 1
        size = chunk if n == 0 else chunk // 2
        return pltpu.make_async_remote_copy(
            relay.at[n, :, pl.ds(0, size)], mixed.at[across, :, pl.ds(j * chunk, size)],
            relay_send.at[n], recv_sem.at[j],
            device_id={"tm": mirror}, device_id_type=MESH)

    def rest(k):
        q, j = place(k)
        at = chunk // 2
        return pltpu.make_async_remote_copy(
            res.at[:, pl.ds(column(q * per + j) + at, at)],
            mixed.at[s, :, pl.ds(column(j) + at, at)],
            send_sem, recv_sem.at[j],
            device_id={"series": q}, device_id_type=MESH)

    def greeting(i):
        if i > len(rounds):
            return
        if i > 0:
            far = rounds[i - 1]
            if far:
                pl.semaphore_wait(met.at[i], heard(far))
            elif group == 2:
                pl.semaphore_wait(met.at[i], 1)
        if i < len(rounds):
            far = rounds[i]
            if far:
                reach(met.at[i + 1], far)
            elif group == 2:
                tell(met.at[i + 1], partner)

    def spread(v):
        return jnp.concatenate([v] * tiles, axis=1)

    greet = min(3, per - 3)

    def step(k, carry):
        @pl.when(k == 0)
        def _():
            fetch(0, lead, 0).wait()

        @pl.when(k == 1)
        def _():
            fetch(0, width - lead, 1).wait()

        @pl.when(k == per - 2)
        def _():
            @pl.when(has_left)
            def _():
                to_right.wait_recv()
                ext[:, :LANE] = halo[0]

            @pl.when(has_right)
            def _():
                to_left.wait_recv()
                ext[:, LANE + width :] = halo[1]

        q, j = place(k)
        base = pl.multiple_of(q * quarter + j * chunk, chunk)
        v = ext[:, pl.ds(base, chunk + 2 * LANE)]
        moved = pltpu.roll(v, chunk + LANE + HALF, 1)
        lines = jnp.concatenate([moved[:, n * LANE : (n + 2) * LANE] for n in range(tiles)], axis=0)
        out = jnp.dot(lines, wts[...], precision=lax.Precision.HIGHEST, preferred_element_type=f32)
        sm = jnp.concatenate([out[n * rows : (n + 1) * rows, :LANE] for n in range(tiles)], axis=1)
        sl = jnp.concatenate([out[n * rows : (n + 1) * rows, LANE:] for n in range(tiles)], axis=1)
        moment = base + lax.broadcasted_iota(jnp.int32, (rows, chunk), 1)
        low = moment - spread(ends[0])
        high = moment - spread(ends[1])
        coef = held(v, base)
        inside = (low >= 0) & (high < 0)
        below = low < HALF
        above = high >= -HALF
        along = jnp.where(below, low - HALF, high + HALF + 1).astype(f32)
        lv = jnp.where(below, spread(coef[0]), spread(coef[3]))
        tl = jnp.where(below, spread(coef[1]), spread(coef[4]))
        bd = jnp.where(below, spread(coef[2]), spread(coef[5]))
        end = below | above
        sm = jnp.where(end, lv + tl * along + bd * (along * along - CENTRE_SQ), sm)
        sl = jnp.where(end, HALF * (tl + 2.0 * along * bd), sl)
        sm = jnp.where(inside, sm, 0.0)
        smooth[:, pl.ds(base, chunk)] = sm
        slope[:, pl.ds(base, chunk)] = jnp.where(inside, sl, 0.0)
        rs = jnp.where(inside, v[:, LANE : LANE + chunk] - sm, 0.0)

        @pl.when(k < sends)
        def _():
            res[:, pl.ds(base, chunk)] = rs

        @pl.when(k >= sends)
        def _():
            mixed[s, :, pl.ds(pl.multiple_of(j * chunk, chunk), chunk)] = rs

        @pl.when(k == 0)
        def _():
            pl.semaphore_wait(barrier, n_s - 1 + group - 1 + heard(group))
            if group == 2:
                tell(met.at[0], partner)
            reach(met.at[0], group)

        @pl.when(k == greet)
        def _():
            pl.semaphore_wait(met.at[0], group - 1 + heard(group))

            @pl.when(has_right)
            def _():
                to_right.start()

            @pl.when(has_left)
            def _():
                to_left.start()

            greeting(0)

        @pl.when(k == max(detour, greet + 1))
        def _():
            greeting(1)

        direct = (k >= 1) & (k <= sends)
        if swaps:
            direct &= jnp.logical_not(((k == detour + 1) & whole_from) | ((k == detour + 2) & half_from))

        @pl.when(direct)
        def _():
            transfer(k - 1).start()

        if swaps:
            @pl.when((k == detour + 1) & whole_from)
            def _():
                away(k - 1, 0).start()

            @pl.when((k == detour + 2) & half_from)
            def _():
                away(k - 1, 1).start()
                rest(k - 1).start()

        return carry

    lax.fori_loop(0, steps, step, 0)

    def pass_on(n):
        def move():
            away(detour + n, n).wait_recv()
            onward(n).start()
        return move

    if swaps:
        pl.when(whole_to)(pass_on(0))
        pl.when(half_to)(pass_on(1))

    def arrival(i):
        j = (i + 1) % per
        block = mixed.at[pl.ds(0, n_s - 1), :, pl.ds(pl.multiple_of(j * chunk, chunk), chunk)]
        return pltpu.make_async_remote_copy(
            block, block, send_sem, recv_sem.at[j],
            device_id={"series": lax.rem(s + 1, n_s)}, device_id_type=MESH)

    half = rows // 2
    left_half = lax.broadcasted_iota(jnp.int32, (half, 2 * total), 1) < total

    def pack(v):
        return jnp.where(left_half, v[:half], v[half:])

    gram = jnp.zeros((2 * total, 2 * total), f32)
    for i in range(per):
        greeting(i + 2)
        arrival(i).wait_recv()
        j = (i + 1) % per
        x = jnp.concatenate(
            [mixed[g, :, pl.ds(pl.multiple_of(j * chunk, chunk), chunk)] for g in range(n_s)], axis=0)
        hi = x.astype(jnp.bfloat16)
        lo = (x - hi.astype(f32)).astype(jnp.bfloat16)
        z = jnp.concatenate([hi, lo], axis=0)
        gram = gram + lax.dot_general(z, z, (((1,), (1,)), ((), ())), preferred_element_type=f32)
    for i in range(per + 2, len(rounds) + 1):
        greeting(i)
    both = gram[:total] + gram[total:]
    both = both + pltpu.roll(both, total, 1)
    for g in range(n_s):
        part[g] = pack(both[g * rows : (g + 1) * rows])

    here = t * n_s + s
    peers = n_t * n_s - 1
    turn = (lax.rem(t, group) * pairs + lax.div(t, group)) * n_s + s

    def share(i):
        i = jnp.where(i < turn, i, i + 1)
        row_of, to_s = lax.div(i, n_s), lax.rem(i, n_s)
        to_t = lax.rem(row_of, pairs) * group + lax.div(row_of, pairs)
        return pltpu.make_async_remote_copy(
            part.at[to_s], shares.at[here], share_sem.at[0], share_sem.at[1],
            device_id={"tm": to_t, "series": to_s}, device_id_type=MESH)

    def spread_shares(i, carry):
        share(i).start()
        return carry

    lax.fori_loop(0, peers, spread_shares, 0)
    shares[here] = part[s]

    lane = lax.broadcasted_iota(jnp.int32, (rows, 2 * total), 1)
    lane = jnp.where(lane < total, lane, lane - total)
    first_k = jnp.zeros((rows, 2 * total), jnp.int32)
    last_k = jnp.zeros((rows, 2 * total), jnp.int32)
    for i in range(total):
        first_k = jnp.where(lane == i, starts[i], first_k)
        last_k = jnp.where(lane == i, stops[i], last_k)
    count = pack((jnp.minimum(last_k, last) - jnp.maximum(first_k, first)).astype(f32))

    sent = res.at[:, pl.ds(0, sends * chunk)]
    pltpu.make_async_remote_copy(
        sent, sent, send_sem, recv_sem.at[0],
        device_id={"series": lax.rem(s + 1, n_s)}, device_id_type=MESH).wait_send()

    @pl.when(has_right)
    def _():
        to_right.wait_send()

    @pl.when(has_left)
    def _():
        to_left.wait_send()

    if swaps:
        pl.when(whole_to)(onward(0).wait_send)
        pl.when(half_to)(onward(1).wait_send)
    others = shares.at[pl.ds(0, peers)]
    shared = pltpu.make_async_remote_copy(
        others, others, share_sem.at[0], share_sem.at[1],
        device_id={"series": lax.rem(s + 1, n_s)}, device_id_type=MESH)
    shared.wait_recv()
    full = shares[0]
    for d in range(1, peers + 1):
        full = full + shares[d]
    full = full / count
    cov[:half] = full[:, :total]
    cov[half:] = pltpu.roll(full, total, 1)[:, :total]
    shared.wait_send()


FLUSHES = 4


def flush(smooth, slope, cov, smooth_out, slope_out, cov_out, sems, cov_sem):
    piece = smooth.shape[1] // FLUSHES
    copies = [pltpu.make_async_copy(cov, cov_out, cov_sem)]
    for i in range(FLUSHES):
        span = pl.ds(i * piece, piece)
        copies.append(pltpu.make_async_copy(smooth.at[:, span], smooth_out.at[:, span], sems.at[2 * i]))
        copies.append(pltpu.make_async_copy(slope.at[:, span], slope_out.at[:, span], sems.at[2 * i + 1]))
    for copy in copies:
        copy.start()
    for copy in copies:
        copy.wait()


def solution(mesh):
    n_t, n_s = mesh.shape["tm"], mesh.shape["series"]

    def shards(signal, valid_start, valid_end):
        rows, width = signal.shape
        total = rows * n_s
        quarter = width // n_s
        chunk = chunk_of(quarter)
        per = quarter // chunk
        f32 = jnp.float32
        dma = pltpu.SemaphoreType.DMA
        kept = pl.pallas_call(
            functools.partial(kernel, n_s, n_t, rows, width, chunk),
            out_shape=(
                jax.ShapeDtypeStruct((rows, width), f32),
                jax.ShapeDtypeStruct((rows, width), f32),
                jax.ShapeDtypeStruct((rows, total), f32),
            ),
            in_specs=[pl.BlockSpec(memory_space=pltpu.HBM)] * 3,
            out_specs=(pl.BlockSpec(memory_space=pltpu.VMEM),) * 3,
            scratch_shapes=[
                pltpu.SMEM((total,), jnp.int32),
                pltpu.SMEM((total,), jnp.int32),
                pltpu.VMEM((rows, width + 2 * LANE), f32),
                pltpu.VMEM((2 * LANE, 2 * LANE), f32),
                pltpu.VMEM((2, rows, LANE), jnp.int32),
                pltpu.VMEM((rows, width), f32),
                pltpu.VMEM((n_s, rows, quarter), f32),
                pltpu.VMEM((2, rows, LANE), f32),
                pltpu.VMEM((n_s, rows // 2, 2 * total), f32),
                pltpu.VMEM((n_t * n_s, rows // 2, 2 * total), f32),
                pltpu.VMEM((2, rows, chunk), f32),
                dma((2,)),
                dma((2,)),
                dma((2,)),
                dma((2,)),
                dma,
                dma((per,)),
                dma((2,)),
                pltpu.SemaphoreType.REGULAR((n_t.bit_length() + 1,)),
                dma((2,)),
                dma((2,)),
            ],
            compiler_params=pltpu.CompilerParams(
                collective_id=0, has_side_effects=True, vmem_limit_bytes=67043328 - 8 * rows * width - 12 * 1024 * 1024
            ),
        )(*[pltpu.with_memory_space_constraint(v, pltpu.HBM) for v in (valid_start, valid_end)], signal)
        return pl.pallas_call(
            flush,
            out_shape=tuple(jax.ShapeDtypeStruct(v.shape, f32) for v in kept),
            in_specs=[pl.BlockSpec(memory_space=pltpu.VMEM)] * 3,
            out_specs=(pl.BlockSpec(memory_space=pltpu.HBM),) * 3,
            scratch_shapes=[dma((2 * FLUSHES,)), dma],
            compiler_params=pltpu.CompilerParams(vmem_limit_bytes=1024 * 1024),
        )(*kept)

    in_specs = (P("series", "tm"), P(), P())
    out_specs = (P("series", "tm"), P("series", "tm"), P("series", None))
    return jax.shard_map(shards, mesh=mesh, in_specs=in_specs, out_specs=out_specs, check_vma=False)
```

```python
import functools

import jax
import jax.numpy as jnp
from jax import lax
from jax.experimental import pallas as pl
from jax.experimental.pallas import tpu as pltpu
from jax.sharding import PartitionSpec as P

HALF = 16
LANE = 128
TAPS = 2 * HALF + 1
SECOND = float(sum(j * j for j in range(-HALF, HALF + 1)))
CENTRE_SQ = SECOND / TAPS
FOURTH = float(sum((j * j - CENTRE_SQ) ** 2 for j in range(-HALF, HALF + 1)))
MESH = pl.DeviceIdType.MESH


def chunk_of(quarter):
    chunk = 1024
    while quarter % chunk:
        chunk //= 2
    return chunk


def kernel(
    n_s, n_t, rows, width, chunk,
    start_hbm, end_hbm, sig_hbm,
    smooth, slope, shares, count,
    starts, stops, ext, wts, ends, res, mixed, halo, part, relay,
    load_sem, bound_sem, halo_send, halo_recv, send_sem, recv_sem, share_sem, met, relay_send, relay_recv,
):
    s = lax.axis_index("series")
    t = lax.axis_index("tm")
    quarter = width // n_s
    per = quarter // chunk
    steps = n_s * per
    sends = (n_s - 1) * per
    total = n_s * rows
    tiles = chunk // LANE
    group = 2 - n_t % 2
    pairs = n_t // group
    rounds = []
    far = 2 * group
    while far < n_t:
        rounds.append(far)
        far *= 2
    rounds.append(0)
    swaps = n_s == 4 and group == 2 and len(rounds) > 1 and per >= 8
    f32 = jnp.float32

    def offset(qi):
        if n_s == 4:
            odd = lax.rem(s, 2)
            return jnp.where(qi == 0, 2, jnp.where(qi == 1, 3 - 2 * odd, jnp.where(qi == 2, 1 + 2 * odd, 0)))
        return lax.rem(qi + 1, n_s)

    def fetch(at, size, sem):
        return pltpu.make_async_copy(
            sig_hbm.at[:, pl.ds(pl.multiple_of(at, LANE), size)],
            ext.at[:, pl.ds(pl.multiple_of(at + LANE, LANE), size)],
            load_sem.at[sem])

    head = lax.rem(s + offset(0), n_s) * quarter
    lead = min(chunk + 2 * LANE, quarter - chunk + LANE)
    before = chunk - LANE
    after = quarter - before - lead
    fetch(head + before, lead, 0).start()

    partner = t + 1 - 2 * lax.rem(t, 2)

    def tell(sem, at, ok=None):
        def signal():
            pl.semaphore_signal(sem, inc=1, device_id={"tm": at}, device_id_type=MESH)
        if ok is None:
            signal()
        else:
            pl.when(ok)(signal)

    def reach(sem, far):
        tell(sem, t - far, t >= far)
        tell(sem, t + far, t + far < n_t)

    def heard(far):
        return (t >= far).astype(jnp.int32) + (t + far < n_t).astype(jnp.int32)

    barrier = pltpu.get_barrier_semaphore()
    for d in range(1, n_s):
        pl.semaphore_signal(barrier, inc=1, device_id={"series": lax.rem(s + d, n_s)}, device_id_type=MESH)
    if group == 2:
        tell(barrier, partner)
    reach(barrier, group)

    limits = [
        pltpu.make_async_copy(start_hbm, starts, bound_sem.at[0]),
        pltpu.make_async_copy(end_hbm, stops, bound_sem.at[1]),
    ]
    for limit in limits:
        limit.start()
    fetch(head, before, 1).start()
    if after:
        fetch(head + before + lead, after, 1).start()
    for qi in range(1, n_s):
        fetch(lax.rem(s + offset(qi), n_s) * quarter, quarter, 1).start()

    tap = lax.broadcasted_iota(jnp.int32, (2 * LANE, LANE), 0) - lax.broadcasted_iota(jnp.int32, (2 * LANE, LANE), 1) - HALF
    near = (tap >= -HALF) & (tap <= HALF)
    tap = tap.astype(f32)
    wts[:, :LANE] = jnp.where(near, 1.0 / TAPS - (tap * tap - CENTRE_SQ) * (CENTRE_SQ / FOURTH), 0.0)
    wts[:, LANE:] = jnp.where(near, tap * (HALF / SECOND), 0.0)
    ext[:, :LANE] = jnp.zeros((rows, LANE), f32)
    ext[:, LANE + width :] = jnp.zeros((rows, LANE), f32)

    for limit in limits:
        limit.wait()
    row = lax.broadcasted_iota(jnp.int32, (rows, LANE), 0)
    begin = t * width
    first = jnp.zeros((rows, LANE), jnp.int32)
    last = jnp.zeros((rows, LANE), jnp.int32)
    for i in range(rows):
        first = jnp.where(row == i, starts[s * rows + i], first)
        last = jnp.where(row == i, stops[s * rows + i], last)
    ends[0] = first - begin
    ends[1] = last - begin

    def held(v, base):
        lanes = lax.broadcasted_iota(jnp.int32, (rows, LANE), 1)
        found = []
        for spot in (ends[0] + LANE - base, ends[1] - TAPS + LANE - base):
            tile = lax.shift_right_arithmetic(spot, LANE.bit_length() - 1)
            pair = [jnp.zeros((rows, LANE), f32)] * 2
            for n in range(tiles + 1):
                here = tile == n
                for w in range(2):
                    pair[w] = jnp.where(here, v[:, (n + w) * LANE : (n + w + 1) * LANE], pair[w])
            j = lanes - (spot - tile * LANE + HALF)
            sums = []
            for j, win in ((j, pair[0]), (j + LANE, pair[1])):
                win = jnp.where((j >= -HALF) & (j <= HALF), win, 0.0)
                j = j.astype(f32)
                sums.append((win, win * j, win * (j * j - CENTRE_SQ)))
            for m, scale in enumerate((1.0 / TAPS, 1.0 / SECOND, 1.0 / FOURTH)):
                value = jnp.sum(sums[0][m] + sums[1][m], axis=1, keepdims=True) * scale
                found.append(jnp.broadcast_to(value, (rows, LANE)))
        return found

    right, left = lax.rem(t + 1, n_t), lax.rem(t + n_t - 1, n_t)
    to_right = pltpu.make_async_remote_copy(
        ext.at[:, pl.ds(width, LANE)], halo.at[0], halo_send.at[0], halo_recv.at[0],
        device_id={"tm": right}, device_id_type=MESH)
    to_left = pltpu.make_async_remote_copy(
        ext.at[:, pl.ds(LANE, LANE)], halo.at[1], halo_send.at[1], halo_recv.at[1],
        device_id={"tm": left}, device_id_type=MESH)
    has_right, has_left = t < n_t - 1, t > 0

    mirror = t + group * (pairs - 1 - 2 * lax.div(t, group))
    gap = lax.div(t - mirror, group)
    whole_from, whole_to = gap == 3, gap == -3
    half_from, half_to = gap == 1, gap == -1
    side_from, side_to = lax.rem(t, 2) == 1, lax.rem(t, 2) == 0
    detour = per + 2
    lag = per
    across = lax.rem(s + offset(1), n_s)

    def place(k):
        qi = k // per
        q = lax.rem(s + offset(qi), n_s)
        j = lax.rem(lax.rem(k, per) + 1, per)
        return q, j

    def transfer(k):
        q, j = place(k)
        return pltpu.make_async_remote_copy(
            res.at[:, pl.ds(pl.multiple_of(q * quarter + j * chunk, chunk), chunk)],
            mixed.at[s, :, pl.ds(pl.multiple_of(j * chunk, chunk), chunk)],
            send_sem, recv_sem.at[j],
            device_id={"series": q}, device_id_type=MESH)

    def column(j):
        return pl.multiple_of(j * chunk, chunk)

    def away(k, n):
        q, j = place(k)
        size = chunk if n == 0 else chunk // 2
        return pltpu.make_async_remote_copy(
            res.at[:, pl.ds(column(q * per + j), size)], relay.at[n, :, pl.ds(0, size)],
            send_sem, relay_recv.at[n],
            device_id={"series": across, "tm": mirror}, device_id_type=MESH)

    def onward(n):
        j = detour + n - per + 1
        size = chunk if n == 0 else chunk // 2
        return pltpu.make_async_remote_copy(
            relay.at[n, :, pl.ds(0, size)], mixed.at[across, :, pl.ds(j * chunk, size)],
            relay_send.at[n], recv_sem.at[j],
            device_id={"tm": mirror}, device_id_type=MESH)

    def aside():
        q, j = place(detour - 1)
        return pltpu.make_async_remote_copy(
            res.at[:, pl.ds(column(q * per + j), chunk // 2)], relay.at[2, :, pl.ds(0, chunk // 2)],
            send_sem, relay_recv.at[2],
            device_id={"tm": partner}, device_id_type=MESH)

    def over():
        j = detour - per
        return pltpu.make_async_remote_copy(
            relay.at[2, :, pl.ds(0, chunk // 2)], mixed.at[s, :, pl.ds(j * chunk, chunk // 2)],
            relay_send.at[2], recv_sem.at[j],
            device_id={"series": across, "tm": partner}, device_id_type=MESH)

    def rest(k):
        q, j = place(k)
        at = chunk // 2
        return pltpu.make_async_remote_copy(
            res.at[:, pl.ds(column(q * per + j) + at, at)],
            mixed.at[s, :, pl.ds(column(j) + at, at)],
            send_sem, recv_sem.at[j],
            device_id={"series": q}, device_id_type=MESH)

    def greeting(i):
        if i > len(rounds):
            return
        if i > 0:
            far = rounds[i - 1]
            if far:
                pl.semaphore_wait(met.at[i], heard(far))
            elif group == 2:
                pl.semaphore_wait(met.at[i], 1)
        if i < len(rounds):
            far = rounds[i]
            if far:
                reach(met.at[i + 1], far)
            elif group == 2:
                tell(met.at[i + 1], partner)

    def spread(v):
        return jnp.concatenate([v] * tiles, axis=1)

    greet = min(3, per - 3)

    def step(k, carry):
        @pl.when(k == 0)
        def _():
            fetch(0, lead, 0).wait()

        @pl.when(k == 1)
        def _():
            fetch(0, width - lead, 1).wait()

        @pl.when(k == per - 2)
        def _():
            @pl.when(has_left)
            def _():
                to_right.wait_recv()
                ext[:, :LANE] = halo[0]

            @pl.when(has_right)
            def _():
                to_left.wait_recv()
                ext[:, LANE + width :] = halo[1]

        q, j = place(k)
        base = pl.multiple_of(q * quarter + j * chunk, chunk)
        v = ext[:, pl.ds(base, chunk + 2 * LANE)]
        moved = pltpu.roll(v, chunk + LANE + HALF, 1)
        lines = jnp.concatenate([moved[:, n * LANE : (n + 2) * LANE] for n in range(tiles)], axis=0)
        out = jnp.dot(lines, wts[...], precision=lax.Precision.HIGHEST, preferred_element_type=f32)
        sm = jnp.concatenate([out[n * rows : (n + 1) * rows, :LANE] for n in range(tiles)], axis=1)
        sl = jnp.concatenate([out[n * rows : (n + 1) * rows, LANE:] for n in range(tiles)], axis=1)
        moment = base + lax.broadcasted_iota(jnp.int32, (rows, chunk), 1)
        low = moment - spread(ends[0])
        high = moment - spread(ends[1])
        coef = held(v, base)
        inside = (low >= 0) & (high < 0)
        below = low < HALF
        above = high >= -HALF
        along = jnp.where(below, low - HALF, high + HALF + 1).astype(f32)
        lv = jnp.where(below, spread(coef[0]), spread(coef[3]))
        tl = jnp.where(below, spread(coef[1]), spread(coef[4]))
        bd = jnp.where(below, spread(coef[2]), spread(coef[5]))
        end = below | above
        sm = jnp.where(end, lv + tl * along + bd * (along * along - CENTRE_SQ), sm)
        sl = jnp.where(end, HALF * (tl + 2.0 * along * bd), sl)
        sm = jnp.where(inside, sm, 0.0)
        smooth[:, pl.ds(base, chunk)] = sm
        slope[:, pl.ds(base, chunk)] = jnp.where(inside, sl, 0.0)
        rs = jnp.where(inside, v[:, LANE : LANE + chunk] - sm, 0.0)

        @pl.when(k < sends)
        def _():
            res[:, pl.ds(base, chunk)] = rs

        @pl.when(k >= sends)
        def _():
            mixed[s, :, pl.ds(pl.multiple_of(j * chunk, chunk), chunk)] = rs

        @pl.when(k == 0)
        def _():
            pl.semaphore_wait(barrier, n_s - 1 + group - 1 + heard(group))
            if group == 2:
                tell(met.at[0], partner)
            reach(met.at[0], group)

        @pl.when(k == greet)
        def _():
            pl.semaphore_wait(met.at[0], group - 1 + heard(group))

            @pl.when(has_right)
            def _():
                to_right.start()

            @pl.when(has_left)
            def _():
                to_left.start()

            greeting(0)

        @pl.when(k == max(detour, greet + 1))
        def _():
            greeting(1)

        if not swaps:
            @pl.when((k >= 1) & (k <= sends))
            def _():
                transfer(k - 1).start()

            return carry

        @pl.when((k == detour) & side_from)
        def _():
            aside().start()

        @pl.when((k == detour + 1) & whole_from)
        def _():
            away(k - 1, 0).start()

        @pl.when((k == detour + 2) & half_from)
        def _():
            away(k - 1, 1).start()

        @pl.when((k == per + lag) & side_to)
        def _():
            aside().wait_recv()
            over().start()

        m = jnp.where(k <= per, k - 1, k - 1 - lag)
        split = ((m == detour - 1) & side_from) | ((m == detour + 1) & half_from)
        ready = ((k >= 1) & (k <= per)) | ((k > per + lag) & (m < sends))

        @pl.when(ready & jnp.logical_not(split | ((m == detour) & whole_from)))
        def _():
            transfer(m).start()

        @pl.when(ready & split)
        def _():
            rest(m).start()

        return carry

    lax.fori_loop(0, steps, step, 0)

    def pass_on(n):
        def move():
            away(detour + n, n).wait_recv()
            onward(n).start()
        return move

    if swaps:
        for m in range(steps - 1 - lag, sends):
            transfer(m).start()
        pl.when(whole_to)(pass_on(0))
        pl.when(half_to)(pass_on(1))

    def arrival(i):
        j = (i + 1) % per
        block = mixed.at[pl.ds(0, n_s - 1), :, pl.ds(pl.multiple_of(j * chunk, chunk), chunk)]
        return pltpu.make_async_remote_copy(
            block, block, send_sem, recv_sem.at[j],
            device_id={"series": lax.rem(s + 1, n_s)}, device_id_type=MESH)

    half = rows // 2
    left_half = lax.broadcasted_iota(jnp.int32, (half, 2 * total), 1) < total

    def pack(v):
        return jnp.where(left_half, v[:half], v[half:])

    gram = jnp.zeros((2 * total, 2 * total), f32)
    for i in range(per):
        greeting(i + 2)
        arrival(i).wait_recv()
        j = (i + 1) % per
        x = jnp.concatenate(
            [mixed[g, :, pl.ds(pl.multiple_of(j * chunk, chunk), chunk)] for g in range(n_s)], axis=0)
        hi = x.astype(jnp.bfloat16)
        lo = (x - hi.astype(f32)).astype(jnp.bfloat16)
        z = jnp.concatenate([hi, lo], axis=0)
        gram = gram + lax.dot_general(z, z, (((1,), (1,)), ((), ())), preferred_element_type=f32)
    for i in range(per + 2, len(rounds) + 1):
        greeting(i)
    both = gram[:total] + gram[total:]
    both = both + pltpu.roll(both, total, 1)
    for g in range(n_s):
        part[g] = pack(both[g * rows : (g + 1) * rows])

    here = t * n_s + s
    peers = n_t * n_s - 1

    def share(to_t, to_s):
        return pltpu.make_async_remote_copy(
            part.at[to_s], shares.at[here], share_sem.at[0], share_sem.at[1],
            device_id={"tm": to_t, "series": to_s}, device_id_type=MESH)

    def spread_shares(i, carry):
        beyond = i - group
        beyond = (1 + lax.rem(beyond, pairs - 1)) * group + lax.div(beyond, pairs - 1)
        to_t = jnp.where(i < group, i, beyond)
        for to_s in range(n_s):
            @pl.when((to_t != t) | (s != to_s))
            def _():
                share(to_t, to_s).start()

        return carry

    lax.fori_loop(0, n_t, spread_shares, 0)
    shares[here] = part[s]

    lane = lax.broadcasted_iota(jnp.int32, (rows, 2 * total), 1)
    lane = jnp.where(lane < total, lane, lane - total)
    first_k = jnp.zeros((rows, 2 * total), jnp.int32)
    last_k = jnp.zeros((rows, 2 * total), jnp.int32)
    for i in range(total):
        first_k = jnp.where(lane == i, starts[i], first_k)
        last_k = jnp.where(lane == i, stops[i], last_k)
    count[...] = pack((jnp.minimum(last_k, last) - jnp.maximum(first_k, first)).astype(f32))

    sent = res.at[:, pl.ds(0, sends * chunk)]
    pltpu.make_async_remote_copy(
        sent, sent, send_sem, recv_sem.at[0],
        device_id={"series": lax.rem(s + 1, n_s)}, device_id_type=MESH).wait_send()

    @pl.when(has_right)
    def _():
        to_right.wait_send()

    @pl.when(has_left)
    def _():
        to_left.wait_send()

    if swaps:
        pl.when(whole_to)(onward(0).wait_send)
        pl.when(half_to)(onward(1).wait_send)
        pl.when(side_to)(over().wait_send)
    others = shares.at[pl.ds(0, peers)]
    shared = pltpu.make_async_remote_copy(
        others, others, share_sem.at[0], share_sem.at[1],
        device_id={"series": lax.rem(s + 1, n_s)}, device_id_type=MESH)
    shared.wait_recv()
    shared.wait_send()


FLUSHES = 1


def flush(smooth, slope, shares, count, smooth_out, slope_out, cov_out, cov, sems, cov_sem):
    piece = smooth.shape[1] // FLUSHES
    copies = []
    for i in range(FLUSHES):
        span = pl.ds(i * piece, piece)
        copies.append(pltpu.make_async_copy(smooth.at[:, span], smooth_out.at[:, span], sems.at[2 * i]))
        copies.append(pltpu.make_async_copy(slope.at[:, span], slope_out.at[:, span], sems.at[2 * i + 1]))
    for copy in copies:
        copy.start()
    full = shares[0]
    for d in range(1, shares.shape[0]):
        full = full + shares[d]
    full = full / count[...]
    half, total = full.shape[0], full.shape[1] // 2
    cov[:half] = full[:, :total]
    cov[half:] = pltpu.roll(full, total, 1)[:, :total]
    last = pltpu.make_async_copy(cov, cov_out, cov_sem)
    last.start()
    copies.append(last)
    for copy in copies:
        copy.wait()


def solution(mesh):
    n_t, n_s = mesh.shape["tm"], mesh.shape["series"]

    def shards(signal, valid_start, valid_end):
        rows, width = signal.shape
        total = rows * n_s
        quarter = width // n_s
        chunk = chunk_of(quarter)
        per = quarter // chunk
        f32 = jnp.float32
        dma = pltpu.SemaphoreType.DMA
        kept = pl.pallas_call(
            functools.partial(kernel, n_s, n_t, rows, width, chunk),
            out_shape=(
                jax.ShapeDtypeStruct((rows, width), f32),
                jax.ShapeDtypeStruct((rows, width), f32),
                jax.ShapeDtypeStruct((n_t * n_s, rows // 2, 2 * total), f32),
                jax.ShapeDtypeStruct((rows // 2, 2 * total), f32),
            ),
            in_specs=[pl.BlockSpec(memory_space=pltpu.HBM)] * 3,
            out_specs=(pl.BlockSpec(memory_space=pltpu.VMEM),) * 4,
            scratch_shapes=[
                pltpu.SMEM((total,), jnp.int32),
                pltpu.SMEM((total,), jnp.int32),
                pltpu.VMEM((rows, width + 2 * LANE), f32),
                pltpu.VMEM((2 * LANE, 2 * LANE), f32),
                pltpu.VMEM((2, rows, LANE), jnp.int32),
                pltpu.VMEM((rows, width), f32),
                pltpu.VMEM((n_s, rows, quarter), f32),
                pltpu.VMEM((2, rows, LANE), f32),
                pltpu.VMEM((n_s, rows // 2, 2 * total), f32),
                pltpu.VMEM((3, rows, chunk), f32),
                dma((2,)),
                dma((2,)),
                dma((2,)),
                dma((2,)),
                dma,
                dma((per,)),
                dma((2,)),
                pltpu.SemaphoreType.REGULAR((max(n_t.bit_length() - 1, 3),)),
                dma((3,)),
                dma((3,)),
            ],
            compiler_params=pltpu.CompilerParams(
                collective_id=0, has_side_effects=True, vmem_limit_bytes=67043328 - 8 * rows * width - 12 * 1024 * 1024
            ),
        )(*[pltpu.with_memory_space_constraint(v, pltpu.HBM) for v in (valid_start, valid_end)], signal)
        return pl.pallas_call(
            flush,
            out_shape=tuple(jax.ShapeDtypeStruct(v, f32) for v in ((rows, width), (rows, width), (rows, total))),
            in_specs=[pl.BlockSpec(memory_space=pltpu.VMEM)] * 4,
            out_specs=(pl.BlockSpec(memory_space=pltpu.HBM),) * 3,
            scratch_shapes=[pltpu.VMEM((rows, total), f32), dma((2 * FLUSHES,)), dma],
            compiler_params=pltpu.CompilerParams(vmem_limit_bytes=1024 * 1024),
        )(*kept)

    in_specs = (P("series", "tm"), P(), P())
    out_specs = (P("series", "tm"), P("series", "tm"), P("series", None))
    return jax.shard_map(shards, mesh=mesh, in_specs=in_specs, out_specs=out_specs, check_vma=False)
```

```python
import functools

import jax
import jax.numpy as jnp
from jax import lax
from jax.experimental import pallas as pl
from jax.experimental.pallas import tpu as pltpu
from jax.sharding import PartitionSpec as P

HALF = 16
LANE = 128
TAPS = 2 * HALF + 1
SECOND = float(sum(j * j for j in range(-HALF, HALF + 1)))
CENTRE_SQ = SECOND / TAPS
FOURTH = float(sum((j * j - CENTRE_SQ) ** 2 for j in range(-HALF, HALF + 1)))
MESH = pl.DeviceIdType.MESH


def chunk_of(quarter):
    chunk = 1024
    while quarter % chunk:
        chunk //= 2
    return chunk


def rounds_of(n_t):
    far = 2 * (2 - n_t % 2)
    rounds = []
    while far < n_t:
        rounds.append(far)
        far *= 2
    return rounds


def kernel(
    n_s, n_t, rows, width, chunk,
    start_hbm, end_hbm, sig_hbm,
    smooth, slope, shares, count,
    starts, stops, ext, wts, ends, res, mixed, halo, part, summed, relay,
    load_sem, bound_sem, halo_send, halo_recv, send_sem, recv_sem, share_sem, met, relay_send, relay_recv,
):
    s = lax.axis_index("series")
    t = lax.axis_index("tm")
    quarter = width // n_s
    per = quarter // chunk
    steps = n_s * per
    sends = (n_s - 1) * per
    total = n_s * rows
    tiles = chunk // LANE
    group = 2 - n_t % 2
    pairs = n_t // group
    rounds = rounds_of(n_t)
    swaps = n_s == 4 and group == 2 and rounds and per >= 8
    f32 = jnp.float32

    def offset(qi):
        if n_s == 4:
            odd = lax.rem(s, 2)
            return jnp.where(qi == 0, 2, jnp.where(qi == 1, 3 - 2 * odd, jnp.where(qi == 2, 1 + 2 * odd, 0)))
        return lax.rem(qi + 1, n_s)

    def fetch(at, size, sem):
        return pltpu.make_async_copy(
            sig_hbm.at[:, pl.ds(pl.multiple_of(at, LANE), size)],
            ext.at[:, pl.ds(pl.multiple_of(at + LANE, LANE), size)],
            load_sem.at[sem])

    head = lax.rem(s + offset(0), n_s) * quarter
    lead = min(chunk + 2 * LANE, quarter - chunk + LANE)
    before = chunk - LANE
    after = quarter - before - lead
    fetch(head + before, lead, 0).start()

    partner = t + 1 - 2 * lax.rem(t, 2)

    def tell(sem, at, ok=None):
        def signal():
            pl.semaphore_signal(sem, inc=1, device_id={"tm": at}, device_id_type=MESH)
        if ok is None:
            signal()
        else:
            pl.when(ok)(signal)

    def reach(sem, far):
        tell(sem, t - far, t >= far)
        tell(sem, t + far, t + far < n_t)

    def heard(far):
        return (t >= far).astype(jnp.int32) + (t + far < n_t).astype(jnp.int32)

    barrier = pltpu.get_barrier_semaphore()
    for d in range(1, n_s):
        pl.semaphore_signal(barrier, inc=1, device_id={"series": lax.rem(s + d, n_s)}, device_id_type=MESH)
    if group == 2:
        tell(barrier, partner)
    reach(barrier, group)

    limits = [
        pltpu.make_async_copy(start_hbm, starts, bound_sem.at[0]),
        pltpu.make_async_copy(end_hbm, stops, bound_sem.at[1]),
    ]
    for limit in limits:
        limit.start()
    fetch(head, before, 1).start()
    if after:
        fetch(head + before + lead, after, 1).start()
    for qi in range(1, n_s):
        fetch(lax.rem(s + offset(qi), n_s) * quarter, quarter, 1).start()

    tap = lax.broadcasted_iota(jnp.int32, (2 * LANE, LANE), 0) - lax.broadcasted_iota(jnp.int32, (2 * LANE, LANE), 1) - HALF
    near = (tap >= -HALF) & (tap <= HALF)
    tap = tap.astype(f32)
    wts[:, :LANE] = jnp.where(near, 1.0 / TAPS - (tap * tap - CENTRE_SQ) * (CENTRE_SQ / FOURTH), 0.0)
    wts[:, LANE:] = jnp.where(near, tap * (HALF / SECOND), 0.0)
    ext[:, :LANE] = jnp.zeros((rows, LANE), f32)
    ext[:, LANE + width :] = jnp.zeros((rows, LANE), f32)

    for limit in limits:
        limit.wait()
    row = lax.broadcasted_iota(jnp.int32, (rows, LANE), 0)
    begin = t * width
    first = jnp.zeros((rows, LANE), jnp.int32)
    last = jnp.zeros((rows, LANE), jnp.int32)
    for i in range(rows):
        first = jnp.where(row == i, starts[s * rows + i], first)
        last = jnp.where(row == i, stops[s * rows + i], last)
    ends[0] = first - begin
    ends[1] = last - begin

    def held(v, base):
        lanes = lax.broadcasted_iota(jnp.int32, (rows, LANE), 1)
        found = []
        for spot in (ends[0] + LANE - base, ends[1] - TAPS + LANE - base):
            tile = lax.shift_right_arithmetic(spot, LANE.bit_length() - 1)
            pair = [jnp.zeros((rows, LANE), f32)] * 2
            for n in range(tiles + 1):
                here = tile == n
                for w in range(2):
                    pair[w] = jnp.where(here, v[:, (n + w) * LANE : (n + w + 1) * LANE], pair[w])
            j = lanes - (spot - tile * LANE + HALF)
            sums = []
            for j, win in ((j, pair[0]), (j + LANE, pair[1])):
                win = jnp.where((j >= -HALF) & (j <= HALF), win, 0.0)
                j = j.astype(f32)
                sums.append((win, win * j, win * (j * j - CENTRE_SQ)))
            for m, scale in enumerate((1.0 / TAPS, 1.0 / SECOND, 1.0 / FOURTH)):
                value = jnp.sum(sums[0][m] + sums[1][m], axis=1, keepdims=True) * scale
                found.append(jnp.broadcast_to(value, (rows, LANE)))
        return found

    right, left = lax.rem(t + 1, n_t), lax.rem(t + n_t - 1, n_t)
    to_right = pltpu.make_async_remote_copy(
        ext.at[:, pl.ds(width, LANE)], halo.at[0], halo_send.at[0], halo_recv.at[0],
        device_id={"tm": right}, device_id_type=MESH)
    to_left = pltpu.make_async_remote_copy(
        ext.at[:, pl.ds(LANE, LANE)], halo.at[1], halo_send.at[1], halo_recv.at[1],
        device_id={"tm": left}, device_id_type=MESH)
    has_right, has_left = t < n_t - 1, t > 0

    mirror = t + group * (pairs - 1 - 2 * lax.div(t, group))
    gap = lax.div(t - mirror, group)
    whole_from, whole_to = gap == 3, gap == -3
    half_from, half_to = gap == 1, gap == -1
    side_from, side_to = lax.rem(t, 2) == 1, lax.rem(t, 2) == 0
    detour = per + 2
    lag = per
    slip = 3 * chunk // 8
    across = lax.rem(s + offset(1), n_s)

    def place(k):
        qi = k // per
        q = lax.rem(s + offset(qi), n_s)
        j = lax.rem(lax.rem(k, per) + 1, per)
        return q, j

    def transfer(k):
        q, j = place(k)
        return pltpu.make_async_remote_copy(
            res.at[:, pl.ds(pl.multiple_of(q * quarter + j * chunk, chunk), chunk)],
            mixed.at[s, :, pl.ds(pl.multiple_of(j * chunk, chunk), chunk)],
            send_sem, recv_sem.at[j],
            device_id={"series": q}, device_id_type=MESH)

    def column(j):
        return pl.multiple_of(j * chunk, chunk)

    def away(k, n):
        q, j = place(k)
        size = chunk if n == 0 else chunk // 2
        return pltpu.make_async_remote_copy(
            res.at[:, pl.ds(column(q * per + j), size)], relay.at[0, :, pl.ds(0, size)],
            send_sem, relay_recv.at[0],
            device_id={"series": across, "tm": mirror}, device_id_type=MESH)

    def onward(n):
        j = detour + n - per + 1
        size = chunk if n == 0 else chunk // 2
        return pltpu.make_async_remote_copy(
            relay.at[0, :, pl.ds(0, size)], mixed.at[across, :, pl.ds(j * chunk, size)],
            relay_send.at[0], recv_sem.at[j],
            device_id={"tm": mirror}, device_id_type=MESH)

    def aside():
        q, j = place(detour - 1)
        return pltpu.make_async_remote_copy(
            res.at[:, pl.ds(column(q * per + j), slip)], relay.at[1, :, pl.ds(0, slip)],
            send_sem, relay_recv.at[1],
            device_id={"tm": partner}, device_id_type=MESH)

    def over():
        j = detour - per
        return pltpu.make_async_remote_copy(
            relay.at[1, :, pl.ds(0, slip)], mixed.at[s, :, pl.ds(j * chunk, slip)],
            relay_send.at[1], recv_sem.at[j],
            device_id={"series": across, "tm": partner}, device_id_type=MESH)

    def rest(k, at):
        q, j = place(k)
        return pltpu.make_async_remote_copy(
            res.at[:, pl.ds(column(q * per + j) + at, chunk - at)],
            mixed.at[s, :, pl.ds(column(j) + at, chunk - at)],
            send_sem, recv_sem.at[j],
            device_id={"series": q}, device_id_type=MESH)

    def greeting(i):
        if 0 < i <= len(rounds):
            pl.semaphore_wait(met.at[i], heard(rounds[i - 1]))
        if i < len(rounds):
            reach(met.at[i + 1], rounds[i])

    def spread(v):
        return jnp.concatenate([v] * tiles, axis=1)

    greet = min(3, per - 3)

    def step(k, carry):
        @pl.when(k == 0)
        def _():
            fetch(0, lead, 0).wait()

        @pl.when(k == 1)
        def _():
            fetch(0, width - lead, 1).wait()

        @pl.when(k == per - 2)
        def _():
            @pl.when(has_left)
            def _():
                to_right.wait_recv()
                ext[:, :LANE] = halo[0]

            @pl.when(has_right)
            def _():
                to_left.wait_recv()
                ext[:, LANE + width :] = halo[1]

        q, j = place(k)
        base = pl.multiple_of(q * quarter + j * chunk, chunk)
        v = ext[:, pl.ds(base, chunk + 2 * LANE)]
        moved = pltpu.roll(v, chunk + LANE + HALF, 1)
        lines = jnp.concatenate([moved[:, n * LANE : (n + 2) * LANE] for n in range(tiles)], axis=0)
        out = jnp.dot(lines, wts[...], precision=lax.Precision.HIGHEST, preferred_element_type=f32)
        sm = jnp.concatenate([out[n * rows : (n + 1) * rows, :LANE] for n in range(tiles)], axis=1)
        sl = jnp.concatenate([out[n * rows : (n + 1) * rows, LANE:] for n in range(tiles)], axis=1)
        moment = base + lax.broadcasted_iota(jnp.int32, (rows, chunk), 1)
        low = moment - spread(ends[0])
        high = moment - spread(ends[1])
        coef = held(v, base)
        inside = (low >= 0) & (high < 0)
        below = low < HALF
        above = high >= -HALF
        along = jnp.where(below, low - HALF, high + HALF + 1).astype(f32)
        lv = jnp.where(below, spread(coef[0]), spread(coef[3]))
        tl = jnp.where(below, spread(coef[1]), spread(coef[4]))
        bd = jnp.where(below, spread(coef[2]), spread(coef[5]))
        end = below | above
        sm = jnp.where(end, lv + tl * along + bd * (along * along - CENTRE_SQ), sm)
        sl = jnp.where(end, HALF * (tl + 2.0 * along * bd), sl)
        sm = jnp.where(inside, sm, 0.0)
        smooth[:, pl.ds(base, chunk)] = sm
        slope[:, pl.ds(base, chunk)] = jnp.where(inside, sl, 0.0)
        rs = jnp.where(inside, v[:, LANE : LANE + chunk] - sm, 0.0)

        @pl.when(k < sends)
        def _():
            res[:, pl.ds(base, chunk)] = rs

        @pl.when(k >= sends)
        def _():
            mixed[s, :, pl.ds(pl.multiple_of(j * chunk, chunk), chunk)] = rs

        @pl.when(k == 0)
        def _():
            pl.semaphore_wait(barrier, n_s - 1 + group - 1 + heard(group))
            if group == 2:
                tell(met.at[0], partner)
            reach(met.at[0], group)

        @pl.when(k == greet)
        def _():
            pl.semaphore_wait(met.at[0], group - 1 + heard(group))

            @pl.when(has_right)
            def _():
                to_right.start()

            @pl.when(has_left)
            def _():
                to_left.start()

            greeting(0)

        @pl.when(k == max(detour, greet + 1))
        def _():
            greeting(1)

        if not swaps:
            @pl.when((k >= 1) & (k <= sends))
            def _():
                transfer(k - 1).start()

            return carry

        @pl.when((k == detour) & side_from)
        def _():
            aside().start()

        @pl.when((k == detour + 1) & whole_from)
        def _():
            away(k - 1, 0).start()

        @pl.when((k == detour + 2) & half_from)
        def _():
            away(k - 1, 1).start()

        @pl.when((k == per + lag) & side_to)
        def _():
            aside().wait_recv()
            over().start()

        m = jnp.where(k <= per, k - 1, k - 1 - lag)
        fork, split = (m == detour - 1) & side_from, (m == detour + 1) & half_from
        ready = ((k >= 1) & (k <= per)) | ((k > per + lag) & (m < sends))

        @pl.when(ready & jnp.logical_not(fork | split | ((m == detour) & whole_from)))
        def _():
            transfer(m).start()

        @pl.when(ready & fork)
        def _():
            rest(m, slip).start()

        @pl.when(ready & split)
        def _():
            rest(m, chunk // 2).start()

        return carry

    lax.fori_loop(0, steps, step, 0)

    def pass_on(n):
        def move():
            away(detour + n, n).wait_recv()
            onward(n).start()
        return move

    if swaps:
        for m in range(steps - 1 - lag, sends):
            transfer(m).start()
        pl.when(whole_to)(pass_on(0))
        pl.when(half_to)(pass_on(1))

    def arrival(i):
        j = (i + 1) % per
        block = mixed.at[pl.ds(0, n_s - 1), :, pl.ds(pl.multiple_of(j * chunk, chunk), chunk)]
        return pltpu.make_async_remote_copy(
            block, block, send_sem, recv_sem.at[j],
            device_id={"series": lax.rem(s + 1, n_s)}, device_id_type=MESH)

    half = rows // 2
    left_half = lax.broadcasted_iota(jnp.int32, (half, 2 * total), 1) < total

    def pack(v):
        return jnp.where(left_half, v[:half], v[half:])

    gram = jnp.zeros((2 * total, 2 * total), f32)
    for i in range(per):
        greeting(i + 2)
        arrival(i).wait_recv()
        j = (i + 1) % per
        x = jnp.concatenate(
            [mixed[g, :, pl.ds(pl.multiple_of(j * chunk, chunk), chunk)] for g in range(n_s)], axis=0)
        hi = x.astype(jnp.bfloat16)
        lo = (x - hi.astype(f32)).astype(jnp.bfloat16)
        z = jnp.concatenate([hi, lo], axis=0)
        gram = gram + lax.dot_general(z, z, (((1,), (1,)), ((), ())), preferred_element_type=f32)
    for i in range(per + 2, len(rounds) + 1):
        greeting(i)
    both = gram[:total] + gram[total:]
    both = both + pltpu.roll(both, total, 1)
    here = t * n_s + s
    whole = n_t * n_s
    nest = n_t * n_s // 2
    first_in = (t == 0) & (s < 2)

    def early(to_s):
        return pltpu.make_async_remote_copy(
            part.at[to_s], shares.at[here], share_sem.at[0], share_sem.at[1],
            device_id={"tm": 0, "series": to_s}, device_id_type=MESH)

    for g in range(n_s):
        part[g] = pack(both[g * rows : (g + 1) * rows])
        if g < 2:
            @pl.when((t != 0) | (s != g))
            def _():
                early(g).start()


    core = lax.rem(s, 2)
    mate = s + 1 - 2 * core

    def swap(g):
        return pltpu.make_async_remote_copy(
            part.at[g * 2 + 1 - core], summed.at[n_s // 2 + g], load_sem.at[0], load_sem.at[1],
            device_id={"series": mate}, device_id_type=MESH)

    for g in range(n_s // 2):
        swap(g).start()
    got = summed.at[pl.ds(n_s // 2, n_s // 2)]
    both_swaps = pltpu.make_async_remote_copy(
        got, got, load_sem.at[0], load_sem.at[1], device_id={"series": mate}, device_id_type=MESH)
    both_swaps.wait_recv()
    for g in range(n_s // 2):
        summed[g] = part[g * 2 + core] + summed[n_s // 2 + g]

    def share(to_t, to_x):
        return pltpu.make_async_remote_copy(
            summed.at[to_x], shares.at[t * (n_s // 2) + lax.div(s, 2)], share_sem.at[0], share_sem.at[1],
            device_id={"tm": to_t, "series": to_x * 2 + core}, device_id_type=MESH)

    def spread_shares(i, carry):
        beyond = i - group
        beyond = (1 + lax.rem(beyond, pairs - 1)) * group + lax.div(beyond, pairs - 1)
        to_t = jnp.where(i < group, i, beyond)
        for to_x in range(n_s // 2):
            @pl.when(((to_t != t) | (lax.div(s, 2) != to_x)) & ((to_t != 0) | (to_x != 0)))
            def _():
                share(to_t, to_x).start()

        return carry

    lax.fori_loop(0, n_t, spread_shares, 0)
    both_swaps.wait_send()

    @pl.when(first_in)
    def _():
        shares[here] = part[s]

    @pl.when(jnp.logical_not(first_in))
    def _():
        shares[t * (n_s // 2) + lax.div(s, 2)] = summed[lax.div(s, 2)]
        shares[nest:] = jnp.zeros((whole - nest, half, 2 * total), f32)

    lane = lax.broadcasted_iota(jnp.int32, (rows, 2 * total), 1)
    lane = jnp.where(lane < total, lane, lane - total)
    first_k = jnp.zeros((rows, 2 * total), jnp.int32)
    last_k = jnp.zeros((rows, 2 * total), jnp.int32)
    for i in range(total):
        first_k = jnp.where(lane == i, starts[i], first_k)
        last_k = jnp.where(lane == i, stops[i], last_k)
    count[...] = pack((jnp.minimum(last_k, last) - jnp.maximum(first_k, first)).astype(f32))

    sent = res.at[:, pl.ds(0, sends * chunk)]
    pltpu.make_async_remote_copy(
        sent, sent, send_sem, recv_sem.at[0],
        device_id={"series": lax.rem(s + 1, n_s)}, device_id_type=MESH).wait_send()

    @pl.when(has_right)
    def _():
        to_right.wait_send()

    @pl.when(has_left)
    def _():
        to_left.wait_send()

    if swaps:
        pl.when(whole_to)(onward(0).wait_send)
        pl.when(half_to)(onward(1).wait_send)
        pl.when(side_to)(over().wait_send)
    def batch(n):
        block = shares.at[pl.ds(0, n)]
        return pltpu.make_async_remote_copy(
            block, block, share_sem.at[0], share_sem.at[1],
            device_id={"series": lax.rem(s + 1, n_s)}, device_id_type=MESH)

    pl.when(first_in)(batch(whole - 1).wait_recv)
    pl.when(jnp.logical_not(first_in))(batch(nest - 1).wait_recv)
    batch(nest).wait_send()


FLUSHES = 1


def flush(smooth, slope, shares, count, smooth_out, slope_out, cov_out, cov, sems, cov_sem):
    piece = smooth.shape[1] // FLUSHES
    copies = []
    for i in range(FLUSHES):
        span = pl.ds(i * piece, piece)
        copies.append(pltpu.make_async_copy(smooth.at[:, span], smooth_out.at[:, span], sems.at[2 * i]))
        copies.append(pltpu.make_async_copy(slope.at[:, span], slope_out.at[:, span], sems.at[2 * i + 1]))
    for copy in copies:
        copy.start()
    full = shares[0]
    for d in range(1, shares.shape[0]):
        full = full + shares[d]
    full = full / count[...]
    half, total = full.shape[0], full.shape[1] // 2
    cov[:half] = full[:, :total]
    cov[half:] = pltpu.roll(full, total, 1)[:, :total]
    last = pltpu.make_async_copy(cov, cov_out, cov_sem)
    last.start()
    copies.append(last)
    for copy in copies:
        copy.wait()


def solution(mesh):
    n_t, n_s = mesh.shape["tm"], mesh.shape["series"]

    def shards(signal, valid_start, valid_end):
        rows, width = signal.shape
        total = rows * n_s
        quarter = width // n_s
        chunk = chunk_of(quarter)
        per = quarter // chunk
        f32 = jnp.float32
        dma = pltpu.SemaphoreType.DMA
        kept = pl.pallas_call(
            functools.partial(kernel, n_s, n_t, rows, width, chunk),
            out_shape=(
                jax.ShapeDtypeStruct((rows, width), f32),
                jax.ShapeDtypeStruct((rows, width), f32),
                jax.ShapeDtypeStruct((n_t * n_s, rows // 2, 2 * total), f32),
                jax.ShapeDtypeStruct((rows // 2, 2 * total), f32),
            ),
            in_specs=[pl.BlockSpec(memory_space=pltpu.HBM)] * 3,
            out_specs=(pl.BlockSpec(memory_space=pltpu.VMEM),) * 4,
            scratch_shapes=[
                pltpu.SMEM((total,), jnp.int32),
                pltpu.SMEM((total,), jnp.int32),
                pltpu.VMEM((rows, width + 2 * LANE), f32),
                pltpu.VMEM((2 * LANE, 2 * LANE), f32),
                pltpu.VMEM((2, rows, LANE), jnp.int32),
                pltpu.VMEM((rows, width), f32),
                pltpu.VMEM((n_s, rows, quarter), f32),
                pltpu.VMEM((2, rows, LANE), f32),
                pltpu.VMEM((n_s, rows // 2, 2 * total), f32),
                pltpu.VMEM((n_s, rows // 2, 2 * total), f32),
                pltpu.VMEM((2, rows, chunk), f32),
                dma((2,)),
                dma((2,)),
                dma((2,)),
                dma((2,)),
                dma,
                dma((per,)),
                dma((2,)),
                pltpu.SemaphoreType.REGULAR((1 + len(rounds_of(n_t)),)),
                dma((2,)),
                dma((2,)),
            ],
            compiler_params=pltpu.CompilerParams(
                collective_id=0, has_side_effects=True, vmem_limit_bytes=67043328 - 8 * rows * width - 12 * 1024 * 1024
            ),
        )(*[pltpu.with_memory_space_constraint(v, pltpu.HBM) for v in (valid_start, valid_end)], signal)
        return pl.pallas_call(
            flush,
            out_shape=tuple(jax.ShapeDtypeStruct(v, f32) for v in ((rows, width), (rows, width), (rows, total))),
            in_specs=[pl.BlockSpec(memory_space=pltpu.VMEM)] * 4,
            out_specs=(pl.BlockSpec(memory_space=pltpu.HBM),) * 3,
            scratch_shapes=[pltpu.VMEM((rows, total), f32), dma((2 * FLUSHES,)), dma],
            compiler_params=pltpu.CompilerParams(vmem_limit_bytes=1024 * 1024),
        )(*kept)

    in_specs = (P("series", "tm"), P(), P())
    out_specs = (P("series", "tm"), P("series", "tm"), P("series", None))
    return jax.shard_map(shards, mesh=mesh, in_specs=in_specs, out_specs=out_specs, check_vma=False)
```

```python
import functools

import jax
import jax.numpy as jnp
from jax import lax
from jax.experimental import pallas as pl
from jax.experimental.pallas import tpu as pltpu
from jax.sharding import PartitionSpec as P

HALF = 16
LANE = 128
TAPS = 2 * HALF + 1
SECOND = float(sum(j * j for j in range(-HALF, HALF + 1)))
CENTRE_SQ = SECOND / TAPS
FOURTH = float(sum((j * j - CENTRE_SQ) ** 2 for j in range(-HALF, HALF + 1)))
MESH = pl.DeviceIdType.MESH


def chunk_of(quarter):
    chunk = 1024
    while quarter % chunk:
        chunk //= 2
    return chunk


def rounds_of(n_t):
    far = 2 * (2 - n_t % 2)
    rounds = []
    while far < n_t:
        rounds.append(far)
        far *= 2
    return rounds


def kernel(
    n_s, n_t, rows, width, chunk,
    start_hbm, end_hbm, sig_hbm,
    smooth, slope, shares, count,
    starts, stops, ext, wts, ends, res, mixed, halo, part, summed, relay,
    load_sem, bound_sem, halo_send, halo_recv, send_sem, recv_sem, share_sem, met, relay_send, relay_recv,
):
    s = lax.axis_index("series")
    t = lax.axis_index("tm")
    quarter = width // n_s
    per = quarter // chunk
    steps = n_s * per
    sends = (n_s - 1) * per
    total = n_s * rows
    tiles = chunk // LANE
    group = 2 - n_t % 2
    pairs = n_t // group
    rounds = rounds_of(n_t)
    swaps = n_s == 4 and group == 2 and rounds and per >= 8
    f32 = jnp.float32

    def offset(qi):
        if n_s == 4:
            odd = lax.rem(s, 2)
            return jnp.where(qi == 0, 2, jnp.where(qi == 1, 3 - 2 * odd, jnp.where(qi == 2, 1 + 2 * odd, 0)))
        return lax.rem(qi + 1, n_s)

    def fetch(at, size, sem):
        return pltpu.make_async_copy(
            sig_hbm.at[:, pl.ds(pl.multiple_of(at, LANE), size)],
            ext.at[:, pl.ds(pl.multiple_of(at + LANE, LANE), size)],
            load_sem.at[sem])

    head = lax.rem(s + offset(0), n_s) * quarter
    lead = min(chunk + 2 * LANE, quarter - chunk + LANE)
    before = chunk - LANE
    after = quarter - before - lead
    fetch(head + before, lead, 0).start()

    partner = t + 1 - 2 * lax.rem(t, 2)

    def tell(sem, at, ok=None):
        def signal():
            pl.semaphore_signal(sem, inc=1, device_id={"tm": at}, device_id_type=MESH)
        if ok is None:
            signal()
        else:
            pl.when(ok)(signal)

    def reach(sem, far):
        tell(sem, t - far, t >= far)
        tell(sem, t + far, t + far < n_t)

    def heard(far):
        return (t >= far).astype(jnp.int32) + (t + far < n_t).astype(jnp.int32)

    barrier = pltpu.get_barrier_semaphore()
    for d in range(1, n_s):
        pl.semaphore_signal(barrier, inc=1, device_id={"series": lax.rem(s + d, n_s)}, device_id_type=MESH)
    if group == 2:
        tell(barrier, partner)
    reach(barrier, group)

    limits = [
        pltpu.make_async_copy(start_hbm, starts, bound_sem.at[0]),
        pltpu.make_async_copy(end_hbm, stops, bound_sem.at[1]),
    ]
    for limit in limits:
        limit.start()
    fetch(head, before, 1).start()
    if after:
        fetch(head + before + lead, after, 1).start()
    for qi in range(1, n_s):
        fetch(lax.rem(s + offset(qi), n_s) * quarter, quarter, 1).start()

    tap = lax.broadcasted_iota(jnp.int32, (2 * LANE, LANE), 0) - lax.broadcasted_iota(jnp.int32, (2 * LANE, LANE), 1) - HALF
    near = (tap >= -HALF) & (tap <= HALF)
    tap = tap.astype(f32)
    wts[:, :LANE] = jnp.where(near, 1.0 / TAPS - (tap * tap - CENTRE_SQ) * (CENTRE_SQ / FOURTH), 0.0)
    wts[:, LANE:] = jnp.where(near, tap * (HALF / SECOND), 0.0)
    ext[:, :LANE] = jnp.zeros((rows, LANE), f32)
    ext[:, LANE + width :] = jnp.zeros((rows, LANE), f32)

    for limit in limits:
        limit.wait()
    row = lax.broadcasted_iota(jnp.int32, (rows, LANE), 0)
    begin = t * width
    first = jnp.zeros((rows, LANE), jnp.int32)
    last = jnp.zeros((rows, LANE), jnp.int32)
    for i in range(rows):
        first = jnp.where(row == i, starts[s * rows + i], first)
        last = jnp.where(row == i, stops[s * rows + i], last)
    ends[0] = first - begin
    ends[1] = last - begin

    def held(v, base):
        lanes = lax.broadcasted_iota(jnp.int32, (rows, LANE), 1)
        found = []
        for spot in (ends[0] + LANE - base, ends[1] - TAPS + LANE - base):
            tile = lax.shift_right_arithmetic(spot, LANE.bit_length() - 1)
            pair = [jnp.zeros((rows, LANE), f32)] * 2
            for n in range(tiles + 1):
                here = tile == n
                for w in range(2):
                    pair[w] = jnp.where(here, v[:, (n + w) * LANE : (n + w + 1) * LANE], pair[w])
            j = lanes - (spot - tile * LANE + HALF)
            sums = []
            for j, win in ((j, pair[0]), (j + LANE, pair[1])):
                win = jnp.where((j >= -HALF) & (j <= HALF), win, 0.0)
                j = j.astype(f32)
                sums.append((win, win * j, win * (j * j - CENTRE_SQ)))
            for m, scale in enumerate((1.0 / TAPS, 1.0 / SECOND, 1.0 / FOURTH)):
                value = jnp.sum(sums[0][m] + sums[1][m], axis=1, keepdims=True) * scale
                found.append(jnp.broadcast_to(value, (rows, LANE)))
        return found

    right, left = lax.rem(t + 1, n_t), lax.rem(t + n_t - 1, n_t)
    to_right = pltpu.make_async_remote_copy(
        ext.at[:, pl.ds(width, LANE)], halo.at[0], halo_send.at[0], halo_recv.at[0],
        device_id={"tm": right}, device_id_type=MESH)
    to_left = pltpu.make_async_remote_copy(
        ext.at[:, pl.ds(LANE, LANE)], halo.at[1], halo_send.at[1], halo_recv.at[1],
        device_id={"tm": left}, device_id_type=MESH)
    has_right, has_left = t < n_t - 1, t > 0

    mirror = t + group * (pairs - 1 - 2 * lax.div(t, group))
    gap = lax.div(t - mirror, group)
    whole_from, whole_to = gap == 3, gap == -3
    half_from, half_to = gap == 1, gap == -1
    side_from, side_to = lax.rem(t, 2) == 1, lax.rem(t, 2) == 0
    detour = per + 2
    lag = per
    slip = 3 * chunk // 8
    across = lax.rem(s + offset(1), n_s)

    def place(k):
        qi = k // per
        q = lax.rem(s + offset(qi), n_s)
        j = lax.rem(lax.rem(k, per) + 1, per)
        return q, j

    def transfer(k):
        q, j = place(k)
        return pltpu.make_async_remote_copy(
            res.at[:, pl.ds(pl.multiple_of(q * quarter + j * chunk, chunk), chunk)],
            mixed.at[s, :, pl.ds(pl.multiple_of(j * chunk, chunk), chunk)],
            send_sem, recv_sem.at[j],
            device_id={"series": q}, device_id_type=MESH)

    def column(j):
        return pl.multiple_of(j * chunk, chunk)

    def away(k, n):
        q, j = place(k)
        size = chunk if n == 0 else chunk // 2
        return pltpu.make_async_remote_copy(
            res.at[:, pl.ds(column(q * per + j), size)], relay.at[0, :, pl.ds(0, size)],
            send_sem, relay_recv.at[0],
            device_id={"series": across, "tm": mirror}, device_id_type=MESH)

    def onward(n):
        j = detour + n - per + 1
        size = chunk if n == 0 else chunk // 2
        return pltpu.make_async_remote_copy(
            relay.at[0, :, pl.ds(0, size)], mixed.at[across, :, pl.ds(j * chunk, size)],
            relay_send.at[0], recv_sem.at[j],
            device_id={"tm": mirror}, device_id_type=MESH)

    def aside():
        q, j = place(detour - 1)
        return pltpu.make_async_remote_copy(
            res.at[:, pl.ds(column(q * per + j), slip)], relay.at[1, :, pl.ds(0, slip)],
            send_sem, relay_recv.at[1],
            device_id={"tm": partner}, device_id_type=MESH)

    def over():
        j = detour - per
        return pltpu.make_async_remote_copy(
            relay.at[1, :, pl.ds(0, slip)], mixed.at[s, :, pl.ds(j * chunk, slip)],
            relay_send.at[1], recv_sem.at[j],
            device_id={"series": across, "tm": partner}, device_id_type=MESH)

    def rest(k, at):
        q, j = place(k)
        return pltpu.make_async_remote_copy(
            res.at[:, pl.ds(column(q * per + j) + at, chunk - at)],
            mixed.at[s, :, pl.ds(column(j) + at, chunk - at)],
            send_sem, recv_sem.at[j],
            device_id={"series": q}, device_id_type=MESH)

    def greeting(i):
        if 0 < i <= len(rounds):
            pl.semaphore_wait(met.at[i], heard(rounds[i - 1]))
        if i < len(rounds):
            reach(met.at[i + 1], rounds[i])

    def spread(v):
        return jnp.concatenate([v] * tiles, axis=1)

    greet = min(3, per - 3)

    def step(k, carry):
        @pl.when(k == 0)
        def _():
            fetch(0, lead, 0).wait()

        @pl.when(k == 1)
        def _():
            fetch(0, width - lead, 1).wait()

        @pl.when(k == per - 2)
        def _():
            @pl.when(has_left)
            def _():
                to_right.wait_recv()
                ext[:, :LANE] = halo[0]

            @pl.when(has_right)
            def _():
                to_left.wait_recv()
                ext[:, LANE + width :] = halo[1]

        q, j = place(k)
        base = pl.multiple_of(q * quarter + j * chunk, chunk)
        v = ext[:, pl.ds(base, chunk + 2 * LANE)]
        moved = pltpu.roll(v, chunk + LANE + HALF, 1)
        lines = jnp.concatenate([moved[:, n * LANE : (n + 2) * LANE] for n in range(tiles)], axis=0)
        out = jnp.dot(lines, wts[...], precision=lax.Precision.HIGHEST, preferred_element_type=f32)
        sm = jnp.concatenate([out[n * rows : (n + 1) * rows, :LANE] for n in range(tiles)], axis=1)
        sl = jnp.concatenate([out[n * rows : (n + 1) * rows, LANE:] for n in range(tiles)], axis=1)
        moment = base + lax.broadcasted_iota(jnp.int32, (rows, chunk), 1)
        low = moment - spread(ends[0])
        high = moment - spread(ends[1])
        coef = held(v, base)
        inside = (low >= 0) & (high < 0)
        below = low < HALF
        above = high >= -HALF
        along = jnp.where(below, low - HALF, high + HALF + 1).astype(f32)
        lv = jnp.where(below, spread(coef[0]), spread(coef[3]))
        tl = jnp.where(below, spread(coef[1]), spread(coef[4]))
        bd = jnp.where(below, spread(coef[2]), spread(coef[5]))
        end = below | above
        sm = jnp.where(end, lv + tl * along + bd * (along * along - CENTRE_SQ), sm)
        sl = jnp.where(end, HALF * (tl + 2.0 * along * bd), sl)
        sm = jnp.where(inside, sm, 0.0)
        smooth[:, pl.ds(base, chunk)] = sm
        slope[:, pl.ds(base, chunk)] = jnp.where(inside, sl, 0.0)
        rs = jnp.where(inside, v[:, LANE : LANE + chunk] - sm, 0.0)

        @pl.when(k < sends)
        def _():
            res[:, pl.ds(base, chunk)] = rs

        @pl.when(k >= sends)
        def _():
            mixed[s, :, pl.ds(pl.multiple_of(j * chunk, chunk), chunk)] = rs

        @pl.when(k == 0)
        def _():
            pl.semaphore_wait(barrier, n_s - 1 + group - 1 + heard(group))
            if group == 2:
                tell(met.at[0], partner)
            reach(met.at[0], group)

        @pl.when(k == greet)
        def _():
            pl.semaphore_wait(met.at[0], group - 1 + heard(group))

            @pl.when(has_right)
            def _():
                to_right.start()

            @pl.when(has_left)
            def _():
                to_left.start()

            greeting(0)

        @pl.when(k == max(detour, greet + 1))
        def _():
            greeting(1)

        if not swaps:
            @pl.when(k < sends)
            def _():
                transfer(k).start()

            return carry

        @pl.when((k == detour - 1) & side_from)
        def _():
            aside().start()

        @pl.when((k == detour) & whole_from)
        def _():
            away(k, 0).start()

        @pl.when((k == detour + 1) & half_from)
        def _():
            away(k, 1).start()

        @pl.when((k == per + lag) & side_to)
        def _():
            aside().wait_recv()
            over().start()

        m = jnp.where(k < per, k, k - lag)
        fork, split = (m == detour - 1) & side_from, (m == detour + 1) & half_from
        ready = (k < per) | ((k >= per + lag) & (m < sends))

        @pl.when(ready & jnp.logical_not(fork | split | ((m == detour) & whole_from)))
        def _():
            transfer(m).start()

        @pl.when(ready & fork)
        def _():
            rest(m, slip).start()

        @pl.when(ready & split)
        def _():
            rest(m, chunk // 2).start()

        return carry

    lax.fori_loop(0, steps, step, 0)

    def pass_on(n):
        def move():
            away(detour + n, n).wait_recv()
            onward(n).start()
        return move

    if swaps:
        for m in range(steps - lag, sends):
            transfer(m).start()
        pl.when(whole_to)(pass_on(0))
        pl.when(half_to)(pass_on(1))

    def arrival(i):
        j = (i + 1) % per
        block = mixed.at[pl.ds(0, n_s - 1), :, pl.ds(pl.multiple_of(j * chunk, chunk), chunk)]
        return pltpu.make_async_remote_copy(
            block, block, send_sem, recv_sem.at[j],
            device_id={"series": lax.rem(s + 1, n_s)}, device_id_type=MESH)

    half = rows // 2
    left_half = lax.broadcasted_iota(jnp.int32, (half, 2 * total), 1) < total

    def pack(v):
        return jnp.where(left_half, v[:half], v[half:])

    gram = jnp.zeros((2 * total, 2 * total), f32)
    for i in range(per):
        greeting(i + 2)
        arrival(i).wait_recv()
        j = (i + 1) % per
        x = jnp.concatenate(
            [mixed[g, :, pl.ds(pl.multiple_of(j * chunk, chunk), chunk)] for g in range(n_s)], axis=0)
        hi = x.astype(jnp.bfloat16)
        lo = (x - hi.astype(f32)).astype(jnp.bfloat16)
        z = jnp.concatenate([hi, lo], axis=0)
        gram = gram + lax.dot_general(z, z, (((1,), (1,)), ((), ())), preferred_element_type=f32)
    for i in range(per + 2, len(rounds) + 1):
        greeting(i)
    both = gram[:total] + gram[total:]
    both = both + pltpu.roll(both, total, 1)
    here = t * n_s + s
    whole = n_t * n_s
    nest = n_t * n_s // 2
    first_in = (t == 0) & (s < 2)

    def early(to_s):
        return pltpu.make_async_remote_copy(
            part.at[to_s], shares.at[here], share_sem.at[0], share_sem.at[1],
            device_id={"tm": 0, "series": to_s}, device_id_type=MESH)

    for g in range(n_s):
        part[g] = pack(both[g * rows : (g + 1) * rows])
    for g in range(2):
        @pl.when((t != 0) | (s != g))
        def _():
            early(g).start()


    core = lax.rem(s, 2)
    mate = s + 1 - 2 * core

    def swap(g):
        return pltpu.make_async_remote_copy(
            part.at[g * 2 + 1 - core], summed.at[n_s // 2 + g], load_sem.at[0], load_sem.at[1],
            device_id={"series": mate}, device_id_type=MESH)

    for g in range(n_s // 2):
        swap(g).start()
    got = summed.at[pl.ds(n_s // 2, n_s // 2)]
    both_swaps = pltpu.make_async_remote_copy(
        got, got, load_sem.at[0], load_sem.at[1], device_id={"series": mate}, device_id_type=MESH)
    both_swaps.wait_recv()
    for g in range(n_s // 2):
        summed[g] = part[g * 2 + core] + summed[n_s // 2 + g]

    def share(to_t, to_x):
        return pltpu.make_async_remote_copy(
            summed.at[to_x], shares.at[t * (n_s // 2) + lax.div(s, 2)], share_sem.at[0], share_sem.at[1],
            device_id={"tm": to_t, "series": to_x * 2 + core}, device_id_type=MESH)

    def spread_shares(i, carry):
        beyond = i - group
        beyond = (1 + lax.rem(beyond, pairs - 1)) * group + lax.div(beyond, pairs - 1)
        to_t = jnp.where(i < group, i, beyond)
        for to_x in range(n_s // 2):
            @pl.when(((to_t != t) | (lax.div(s, 2) != to_x)) & ((to_t != 0) | (to_x != 0)))
            def _():
                share(to_t, to_x).start()

        return carry

    lax.fori_loop(0, n_t, spread_shares, 0)
    both_swaps.wait_send()

    @pl.when(first_in)
    def _():
        shares[here] = part[s]

    @pl.when(jnp.logical_not(first_in))
    def _():
        shares[t * (n_s // 2) + lax.div(s, 2)] = summed[lax.div(s, 2)]
        shares[nest:] = jnp.zeros((whole - nest, half, 2 * total), f32)

    lane = lax.broadcasted_iota(jnp.int32, (rows, 2 * total), 1)
    lane = jnp.where(lane < total, lane, lane - total)
    first_k = jnp.zeros((rows, 2 * total), jnp.int32)
    last_k = jnp.zeros((rows, 2 * total), jnp.int32)
    for i in range(total):
        first_k = jnp.where(lane == i, starts[i], first_k)
        last_k = jnp.where(lane == i, stops[i], last_k)
    count[...] = pack((jnp.minimum(last_k, last) - jnp.maximum(first_k, first)).astype(f32))

    sent = res.at[:, pl.ds(0, sends * chunk)]
    pltpu.make_async_remote_copy(
        sent, sent, send_sem, recv_sem.at[0],
        device_id={"series": lax.rem(s + 1, n_s)}, device_id_type=MESH).wait_send()

    @pl.when(has_right)
    def _():
        to_right.wait_send()

    @pl.when(has_left)
    def _():
        to_left.wait_send()

    if swaps:
        pl.when(whole_to)(onward(0).wait_send)
        pl.when(half_to)(onward(1).wait_send)
        pl.when(side_to)(over().wait_send)
    def batch(n):
        block = shares.at[pl.ds(0, n)]
        return pltpu.make_async_remote_copy(
            block, block, share_sem.at[0], share_sem.at[1],
            device_id={"series": lax.rem(s + 1, n_s)}, device_id_type=MESH)

    pl.when(first_in)(batch(whole - 1).wait_recv)
    pl.when(jnp.logical_not(first_in))(batch(nest - 1).wait_recv)
    batch(nest).wait_send()


FLUSHES = 1


def flush(smooth, slope, shares, count, smooth_out, slope_out, cov_out, cov, sems, cov_sem):
    piece = smooth.shape[1] // FLUSHES
    copies = []
    for i in range(FLUSHES):
        span = pl.ds(i * piece, piece)
        copies.append(pltpu.make_async_copy(smooth.at[:, span], smooth_out.at[:, span], sems.at[2 * i]))
        copies.append(pltpu.make_async_copy(slope.at[:, span], slope_out.at[:, span], sems.at[2 * i + 1]))
    for copy in copies:
        copy.start()
    full = shares[0]
    for d in range(1, shares.shape[0]):
        full = full + shares[d]
    full = full / count[...]
    half, total = full.shape[0], full.shape[1] // 2
    cov[:half] = full[:, :total]
    cov[half:] = pltpu.roll(full, total, 1)[:, :total]
    last = pltpu.make_async_copy(cov, cov_out, cov_sem)
    last.start()
    copies.append(last)
    for copy in copies:
        copy.wait()


def solution(mesh):
    n_t, n_s = mesh.shape["tm"], mesh.shape["series"]

    def shards(signal, valid_start, valid_end):
        rows, width = signal.shape
        total = rows * n_s
        quarter = width // n_s
        chunk = chunk_of(quarter)
        per = quarter // chunk
        f32 = jnp.float32
        dma = pltpu.SemaphoreType.DMA
        kept = pl.pallas_call(
            functools.partial(kernel, n_s, n_t, rows, width, chunk),
            out_shape=(
                jax.ShapeDtypeStruct((rows, width), f32),
                jax.ShapeDtypeStruct((rows, width), f32),
                jax.ShapeDtypeStruct((n_t * n_s, rows // 2, 2 * total), f32),
                jax.ShapeDtypeStruct((rows // 2, 2 * total), f32),
            ),
            in_specs=[pl.BlockSpec(memory_space=pltpu.HBM)] * 3,
            out_specs=(pl.BlockSpec(memory_space=pltpu.VMEM),) * 4,
            scratch_shapes=[
                pltpu.SMEM((total,), jnp.int32),
                pltpu.SMEM((total,), jnp.int32),
                pltpu.VMEM((rows, width + 2 * LANE), f32),
                pltpu.VMEM((2 * LANE, 2 * LANE), f32),
                pltpu.VMEM((2, rows, LANE), jnp.int32),
                pltpu.VMEM((rows, width), f32),
                pltpu.VMEM((n_s, rows, quarter), f32),
                pltpu.VMEM((2, rows, LANE), f32),
                pltpu.VMEM((n_s, rows // 2, 2 * total), f32),
                pltpu.VMEM((n_s, rows // 2, 2 * total), f32),
                pltpu.VMEM((2, rows, chunk), f32),
                dma((2,)),
                dma((2,)),
                dma((2,)),
                dma((2,)),
                dma,
                dma((per,)),
                dma((2,)),
                pltpu.SemaphoreType.REGULAR((1 + len(rounds_of(n_t)),)),
                dma((2,)),
                dma((2,)),
            ],
            compiler_params=pltpu.CompilerParams(
                collective_id=0, has_side_effects=True, vmem_limit_bytes=67043328 - 8 * rows * width - 12 * 1024 * 1024
            ),
        )(*[pltpu.with_memory_space_constraint(v, pltpu.HBM) for v in (valid_start, valid_end)], signal)
        return pl.pallas_call(
            flush,
            out_shape=tuple(jax.ShapeDtypeStruct(v, f32) for v in ((rows, width), (rows, width), (rows, total))),
            in_specs=[pl.BlockSpec(memory_space=pltpu.VMEM)] * 4,
            out_specs=(pl.BlockSpec(memory_space=pltpu.HBM),) * 3,
            scratch_shapes=[pltpu.VMEM((rows, total), f32), dma((2 * FLUSHES,)), dma],
            compiler_params=pltpu.CompilerParams(vmem_limit_bytes=1024 * 1024),
        )(*kept)

    in_specs = (P("series", "tm"), P(), P())
    out_specs = (P("series", "tm"), P("series", "tm"), P("series", None))
    return jax.shard_map(shards, mesh=mesh, in_specs=in_specs, out_specs=out_specs, check_vma=False)
```

```python
import functools

import jax
import jax.numpy as jnp
from jax import lax
from jax.experimental import pallas as pl
from jax.experimental.pallas import tpu as pltpu
from jax.sharding import PartitionSpec as P

HALF = 16
LANE = 128
TAPS = 2 * HALF + 1
SECOND = float(sum(j * j for j in range(-HALF, HALF + 1)))
CENTRE_SQ = SECOND / TAPS
FOURTH = float(sum((j * j - CENTRE_SQ) ** 2 for j in range(-HALF, HALF + 1)))
MESH = pl.DeviceIdType.MESH


def chunk_of(quarter):
    chunk = 1024
    while quarter % chunk:
        chunk //= 2
    return chunk


def rounds_of(n_t):
    far = 2 * (2 - n_t % 2)
    rounds = []
    while far < n_t:
        rounds.append(far)
        far *= 2
    return rounds


def kernel(
    n_s, n_t, rows, width, chunk,
    start_hbm, end_hbm, sig_hbm,
    smooth, slope, shares, count,
    starts, stops, ext, wts, ends, res, mixed, halo, part, summed, relay,
    load_sem, bound_sem, halo_send, halo_recv, send_sem, recv_sem, share_sem, met, relay_send, relay_recv,
):
    s = lax.axis_index("series")
    t = lax.axis_index("tm")
    quarter = width // n_s
    per = quarter // chunk
    steps = n_s * per
    sends = (n_s - 1) * per
    total = n_s * rows
    tiles = chunk // LANE
    group = 2 - n_t % 2
    pairs = n_t // group
    rounds = rounds_of(n_t)
    swaps = n_s == 4 and group == 2 and rounds and per >= 8
    f32 = jnp.float32

    def offset(qi):
        if n_s == 4:
            odd = lax.rem(s, 2)
            return jnp.where(qi == 0, 2, jnp.where(qi == 1, 3 - 2 * odd, jnp.where(qi == 2, 1 + 2 * odd, 0)))
        return lax.rem(qi + 1, n_s)

    def fetch(at, size, sem):
        return pltpu.make_async_copy(
            sig_hbm.at[:, pl.ds(pl.multiple_of(at, LANE), size)],
            ext.at[:, pl.ds(pl.multiple_of(at + LANE, LANE), size)],
            load_sem.at[sem])

    head = lax.rem(s + offset(0), n_s) * quarter
    lead = min(chunk + 2 * LANE, quarter - chunk + LANE)
    before = chunk - LANE
    after = quarter - before - lead
    fetch(head + before, lead, 0).start()

    partner = t + 1 - 2 * lax.rem(t, 2)

    def tell(sem, at, ok=None):
        def signal():
            pl.semaphore_signal(sem, inc=1, device_id={"tm": at}, device_id_type=MESH)
        if ok is None:
            signal()
        else:
            pl.when(ok)(signal)

    def reach(sem, far):
        tell(sem, t - far, t >= far)
        tell(sem, t + far, t + far < n_t)

    def heard(far):
        return (t >= far).astype(jnp.int32) + (t + far < n_t).astype(jnp.int32)

    barrier = pltpu.get_barrier_semaphore()
    for d in range(1, n_s):
        pl.semaphore_signal(barrier, inc=1, device_id={"series": lax.rem(s + d, n_s)}, device_id_type=MESH)
    if group == 2:
        tell(barrier, partner)
    reach(barrier, group)

    limits = [
        pltpu.make_async_copy(start_hbm, starts, bound_sem.at[0]),
        pltpu.make_async_copy(end_hbm, stops, bound_sem.at[1]),
    ]
    for limit in limits:
        limit.start()
    fetch(head, before, 1).start()
    if after:
        fetch(head + before + lead, after, 1).start()
    for qi in range(1, n_s):
        fetch(lax.rem(s + offset(qi), n_s) * quarter, quarter, 1).start()

    tap = lax.broadcasted_iota(jnp.int32, (2 * LANE, LANE), 0) - lax.broadcasted_iota(jnp.int32, (2 * LANE, LANE), 1) - HALF
    near = (tap >= -HALF) & (tap <= HALF)
    tap = tap.astype(f32)
    wts[:, :LANE] = jnp.where(near, 1.0 / TAPS - (tap * tap - CENTRE_SQ) * (CENTRE_SQ / FOURTH), 0.0)
    wts[:, LANE:] = jnp.where(near, tap * (HALF / SECOND), 0.0)
    ext[:, :LANE] = jnp.zeros((rows, LANE), f32)
    ext[:, LANE + width :] = jnp.zeros((rows, LANE), f32)

    for limit in limits:
        limit.wait()
    row = lax.broadcasted_iota(jnp.int32, (rows, LANE), 0)
    begin = t * width
    first = jnp.zeros((rows, LANE), jnp.int32)
    last = jnp.zeros((rows, LANE), jnp.int32)
    for i in range(rows):
        first = jnp.where(row == i, starts[s * rows + i], first)
        last = jnp.where(row == i, stops[s * rows + i], last)
    ends[0] = first - begin
    ends[1] = last - begin

    def held(v, base):
        lanes = lax.broadcasted_iota(jnp.int32, (rows, LANE), 1)
        found = []
        for spot in (ends[0] + LANE - base, ends[1] - TAPS + LANE - base):
            tile = lax.shift_right_arithmetic(spot, LANE.bit_length() - 1)
            pair = [jnp.zeros((rows, LANE), f32)] * 2
            for n in range(tiles + 1):
                here = tile == n
                for w in range(2):
                    pair[w] = jnp.where(here, v[:, (n + w) * LANE : (n + w + 1) * LANE], pair[w])
            j = lanes - (spot - tile * LANE + HALF)
            sums = []
            for j, win in ((j, pair[0]), (j + LANE, pair[1])):
                win = jnp.where((j >= -HALF) & (j <= HALF), win, 0.0)
                j = j.astype(f32)
                sums.append((win, win * j, win * (j * j - CENTRE_SQ)))
            for m, scale in enumerate((1.0 / TAPS, 1.0 / SECOND, 1.0 / FOURTH)):
                value = jnp.sum(sums[0][m] + sums[1][m], axis=1, keepdims=True) * scale
                found.append(jnp.broadcast_to(value, (rows, LANE)))
        return found

    right, left = lax.rem(t + 1, n_t), lax.rem(t + n_t - 1, n_t)
    to_right = pltpu.make_async_remote_copy(
        ext.at[:, pl.ds(width, LANE)], halo.at[0], halo_send.at[0], halo_recv.at[0],
        device_id={"tm": right}, device_id_type=MESH)
    to_left = pltpu.make_async_remote_copy(
        ext.at[:, pl.ds(LANE, LANE)], halo.at[1], halo_send.at[1], halo_recv.at[1],
        device_id={"tm": left}, device_id_type=MESH)
    has_right, has_left = t < n_t - 1, t > 0

    mirror = t + group * (pairs - 1 - 2 * lax.div(t, group))
    gap = lax.div(t - mirror, group)
    whole_from, whole_to = gap == 3, gap == -3
    half_from, half_to = gap == 1, gap == -1
    side_from, side_to = lax.rem(t, 2) == 1, lax.rem(t, 2) == 0
    detour = per + 2
    lag = per
    slip = 3 * chunk // 8
    across = lax.rem(s + offset(1), n_s)

    def place(k):
        qi = k // per
        q = lax.rem(s + offset(qi), n_s)
        j = lax.rem(lax.rem(k, per) + 1, per)
        return q, j

    def transfer(k):
        q, j = place(k)
        return pltpu.make_async_remote_copy(
            res.at[:, pl.ds(pl.multiple_of(q * quarter + j * chunk, chunk), chunk)],
            mixed.at[s, :, pl.ds(pl.multiple_of(j * chunk, chunk), chunk)],
            send_sem, recv_sem.at[j],
            device_id={"series": q}, device_id_type=MESH)

    def column(j):
        return pl.multiple_of(j * chunk, chunk)

    tail = chunk // 4

    def closing(k, at, size, sem):
        q, j = place(k)
        return pltpu.make_async_remote_copy(
            res.at[:, pl.ds(column(q * per + j) + at, size)], mixed.at[s, :, pl.ds(column(j) + at, size)],
            send_sem, recv_sem.at[sem],
            device_id={"series": q}, device_id_type=MESH)

    def send(k):
        ends_here = lax.rem(k, per) == per - 1

        @pl.when(jnp.logical_not(ends_here))
        def _():
            transfer(k).start()

        @pl.when(ends_here)
        def _():
            closing(k, 0, chunk - tail, 0).start()
            closing(k, chunk - tail, tail, per).start()

    def away(k, n):
        q, j = place(k)
        size = chunk if n == 0 else chunk // 4
        return pltpu.make_async_remote_copy(
            res.at[:, pl.ds(column(q * per + j), size)], relay.at[0, :, pl.ds(0, size)],
            send_sem, relay_recv.at[0],
            device_id={"series": across, "tm": mirror}, device_id_type=MESH)

    def onward(n):
        j = detour + n - per + 1
        size = chunk if n == 0 else chunk // 4
        return pltpu.make_async_remote_copy(
            relay.at[0, :, pl.ds(0, size)], mixed.at[across, :, pl.ds(j * chunk, size)],
            relay_send.at[0], recv_sem.at[j],
            device_id={"tm": mirror}, device_id_type=MESH)

    def aside():
        q, j = place(detour - 1)
        return pltpu.make_async_remote_copy(
            res.at[:, pl.ds(column(q * per + j), slip)], relay.at[1, :, pl.ds(0, slip)],
            send_sem, relay_recv.at[1],
            device_id={"tm": partner}, device_id_type=MESH)

    def over():
        j = detour - per
        return pltpu.make_async_remote_copy(
            relay.at[1, :, pl.ds(0, slip)], mixed.at[s, :, pl.ds(j * chunk, slip)],
            relay_send.at[1], recv_sem.at[j],
            device_id={"series": across, "tm": partner}, device_id_type=MESH)

    def rest(k, at):
        q, j = place(k)
        return pltpu.make_async_remote_copy(
            res.at[:, pl.ds(column(q * per + j) + at, chunk - at)],
            mixed.at[s, :, pl.ds(column(j) + at, chunk - at)],
            send_sem, recv_sem.at[j],
            device_id={"series": q}, device_id_type=MESH)

    def greeting(i):
        if 0 < i <= len(rounds):
            pl.semaphore_wait(met.at[i], heard(rounds[i - 1]))
        if i < len(rounds):
            reach(met.at[i + 1], rounds[i])

    def spread(v):
        return jnp.concatenate([v] * tiles, axis=1)

    greet = min(3, per - 3)

    def step(k, carry):
        @pl.when(k == 0)
        def _():
            fetch(0, lead, 0).wait()

        @pl.when(k == 1)
        def _():
            fetch(0, width - lead, 1).wait()

        @pl.when(k == per - 2)
        def _():
            @pl.when(has_left)
            def _():
                to_right.wait_recv()
                ext[:, :LANE] = halo[0]

            @pl.when(has_right)
            def _():
                to_left.wait_recv()
                ext[:, LANE + width :] = halo[1]

        q, j = place(k)
        base = pl.multiple_of(q * quarter + j * chunk, chunk)
        v = ext[:, pl.ds(base, chunk + 2 * LANE)]
        moved = pltpu.roll(v, chunk + LANE + HALF, 1)
        lines = jnp.concatenate([moved[:, n * LANE : (n + 2) * LANE] for n in range(tiles)], axis=0)
        out = jnp.dot(lines, wts[...], precision=lax.Precision.HIGHEST, preferred_element_type=f32)
        sm = jnp.concatenate([out[n * rows : (n + 1) * rows, :LANE] for n in range(tiles)], axis=1)
        sl = jnp.concatenate([out[n * rows : (n + 1) * rows, LANE:] for n in range(tiles)], axis=1)
        moment = base + lax.broadcasted_iota(jnp.int32, (rows, chunk), 1)
        low = moment - spread(ends[0])
        high = moment - spread(ends[1])
        coef = held(v, base)
        inside = (low >= 0) & (high < 0)
        below = low < HALF
        above = high >= -HALF
        along = jnp.where(below, low - HALF, high + HALF + 1).astype(f32)
        lv = jnp.where(below, spread(coef[0]), spread(coef[3]))
        tl = jnp.where(below, spread(coef[1]), spread(coef[4]))
        bd = jnp.where(below, spread(coef[2]), spread(coef[5]))
        end = below | above
        sm = jnp.where(end, lv + tl * along + bd * (along * along - CENTRE_SQ), sm)
        sl = jnp.where(end, HALF * (tl + 2.0 * along * bd), sl)
        sm = jnp.where(inside, sm, 0.0)
        smooth[:, pl.ds(base, chunk)] = sm
        slope[:, pl.ds(base, chunk)] = jnp.where(inside, sl, 0.0)
        rs = jnp.where(inside, v[:, LANE : LANE + chunk] - sm, 0.0)

        @pl.when(k < sends)
        def _():
            res[:, pl.ds(base, chunk)] = rs

        @pl.when(k >= sends)
        def _():
            mixed[s, :, pl.ds(pl.multiple_of(j * chunk, chunk), chunk)] = rs

        @pl.when(k == 0)
        def _():
            pl.semaphore_wait(barrier, n_s - 1 + group - 1 + heard(group))
            if group == 2:
                tell(met.at[0], partner)
            reach(met.at[0], group)

        @pl.when(k == greet)
        def _():
            pl.semaphore_wait(met.at[0], group - 1 + heard(group))

            @pl.when(has_right)
            def _():
                to_right.start()

            @pl.when(has_left)
            def _():
                to_left.start()

            greeting(0)

        @pl.when(k == max(detour, greet + 1))
        def _():
            greeting(1)

        if not swaps:
            @pl.when(k < sends)
            def _():
                send(k)

            return carry

        @pl.when((k == detour - 1) & side_from)
        def _():
            aside().start()

        @pl.when((k == detour) & whole_from)
        def _():
            away(k, 0).start()

        @pl.when((k == detour + 1) & half_from)
        def _():
            away(k, 1).start()

        @pl.when((k == per + lag) & side_to)
        def _():
            aside().wait_recv()
            over().start()

        m = jnp.where(k < per, k, k - lag)
        fork, split = (m == detour - 1) & side_from, (m == detour + 1) & half_from
        ready = (k < per) | ((k >= per + lag) & (m < sends))

        @pl.when(ready & jnp.logical_not(fork | split | ((m == detour) & whole_from)))
        def _():
            send(m)

        @pl.when(ready & fork)
        def _():
            rest(m, slip).start()

        @pl.when(ready & split)
        def _():
            rest(m, chunk // 4).start()

        return carry

    lax.fori_loop(0, steps, step, 0)

    def pass_on(n):
        def move():
            away(detour + n, n).wait_recv()
            onward(n).start()
        return move

    if swaps:
        for m in range(steps - lag, sends):
            send(m)
        pl.when(whole_to)(pass_on(0))
        pl.when(half_to)(pass_on(1))

    def arrival(at, size, sem):
        block = mixed.at[pl.ds(0, n_s - 1), :, pl.ds(at, size)]
        return pltpu.make_async_remote_copy(
            block, block, send_sem, recv_sem.at[sem],
            device_id={"series": lax.rem(s + 1, n_s)}, device_id_type=MESH)

    half = rows // 2
    left_half = lax.broadcasted_iota(jnp.int32, (half, 2 * total), 1) < total

    def pack(v):
        return jnp.where(left_half, v[:half], v[half:])

    gram = jnp.zeros((2 * total, 2 * total), f32)
    parts = [(j * chunk, chunk, j) for j in range(1, per)]
    parts += [(0, chunk - tail, 0), (chunk - tail, tail, per)]
    for i, (at, size, sem) in enumerate(parts):
        greeting(i + 2)
        arrival(at, size, sem).wait_recv()
        x = jnp.concatenate([mixed[g, :, at : at + size] for g in range(n_s)], axis=0)
        hi = x.astype(jnp.bfloat16)
        lo = (x - hi.astype(f32)).astype(jnp.bfloat16)
        z = jnp.concatenate([hi, lo], axis=0)
        gram = gram + lax.dot_general(z, z, (((1,), (1,)), ((), ())), preferred_element_type=f32)
    for i in range(per + 3, len(rounds) + 1):
        greeting(i)
    both = gram[:total] + gram[total:]
    both = both + pltpu.roll(both, total, 1)
    here = t * n_s + s
    whole = n_t * n_s
    nest = n_t * n_s // 2
    first_in = (t == 0) & (s < 2)

    def early(to_s):
        return pltpu.make_async_remote_copy(
            part.at[to_s], shares.at[here], share_sem.at[0], share_sem.at[1],
            device_id={"tm": 0, "series": to_s}, device_id_type=MESH)

    for g in range(n_s):
        part[g] = pack(both[g * rows : (g + 1) * rows])
    for g in range(2):
        @pl.when((t != 0) | (s != g))
        def _():
            early(g).start()


    core = lax.rem(s, 2)
    mate = s + 1 - 2 * core

    def swap(g):
        return pltpu.make_async_remote_copy(
            part.at[g * 2 + 1 - core], summed.at[n_s // 2 + g], load_sem.at[0], load_sem.at[1],
            device_id={"series": mate}, device_id_type=MESH)

    for g in range(n_s // 2):
        swap(g).start()
    got = summed.at[pl.ds(n_s // 2, n_s // 2)]
    both_swaps = pltpu.make_async_remote_copy(
        got, got, load_sem.at[0], load_sem.at[1], device_id={"series": mate}, device_id_type=MESH)
    both_swaps.wait_recv()
    for g in range(n_s // 2):
        summed[g] = part[g * 2 + core] + summed[n_s // 2 + g]

    def share(to_t, to_x):
        return pltpu.make_async_remote_copy(
            summed.at[to_x], shares.at[t * (n_s // 2) + lax.div(s, 2)], share_sem.at[0], share_sem.at[1],
            device_id={"tm": to_t, "series": to_x * 2 + core}, device_id_type=MESH)

    def spread_shares(i, carry):
        beyond = i - group
        beyond = (1 + lax.rem(beyond, pairs - 1)) * group + lax.div(beyond, pairs - 1)
        to_t = jnp.where(i < group, i, beyond)
        for to_x in range(n_s // 2):
            @pl.when(((to_t != t) | (lax.div(s, 2) != to_x)) & ((to_t != 0) | (to_x != 0)))
            def _():
                share(to_t, to_x).start()

        return carry

    lax.fori_loop(0, n_t, spread_shares, 0)
    both_swaps.wait_send()

    @pl.when(first_in)
    def _():
        shares[here] = part[s]

    @pl.when(jnp.logical_not(first_in))
    def _():
        shares[t * (n_s // 2) + lax.div(s, 2)] = summed[lax.div(s, 2)]
        shares[nest:] = jnp.zeros((whole - nest, half, 2 * total), f32)

    lane = lax.broadcasted_iota(jnp.int32, (rows, 2 * total), 1)
    lane = jnp.where(lane < total, lane, lane - total)
    first_k = jnp.zeros((rows, 2 * total), jnp.int32)
    last_k = jnp.zeros((rows, 2 * total), jnp.int32)
    for i in range(total):
        first_k = jnp.where(lane == i, starts[i], first_k)
        last_k = jnp.where(lane == i, stops[i], last_k)
    count[...] = pack((jnp.minimum(last_k, last) - jnp.maximum(first_k, first)).astype(f32))

    sent = res.at[:, pl.ds(0, sends * chunk)]
    pltpu.make_async_remote_copy(
        sent, sent, send_sem, recv_sem.at[0],
        device_id={"series": lax.rem(s + 1, n_s)}, device_id_type=MESH).wait_send()

    @pl.when(has_right)
    def _():
        to_right.wait_send()

    @pl.when(has_left)
    def _():
        to_left.wait_send()

    if swaps:
        pl.when(whole_to)(onward(0).wait_send)
        pl.when(half_to)(onward(1).wait_send)
        pl.when(side_to)(over().wait_send)
    def batch(n):
        block = shares.at[pl.ds(0, n)]
        return pltpu.make_async_remote_copy(
            block, block, share_sem.at[0], share_sem.at[1],
            device_id={"series": lax.rem(s + 1, n_s)}, device_id_type=MESH)

    pl.when(first_in)(batch(whole - 1).wait_recv)
    pl.when(jnp.logical_not(first_in))(batch(nest - 1).wait_recv)
    batch(nest).wait_send()


FLUSHES = 1


def flush(smooth, slope, shares, count, smooth_out, slope_out, cov_out, cov, sems, cov_sem):
    piece = smooth.shape[1] // FLUSHES
    copies = []
    for i in range(FLUSHES):
        span = pl.ds(i * piece, piece)
        copies.append(pltpu.make_async_copy(smooth.at[:, span], smooth_out.at[:, span], sems.at[2 * i]))
        copies.append(pltpu.make_async_copy(slope.at[:, span], slope_out.at[:, span], sems.at[2 * i + 1]))
    for copy in copies:
        copy.start()
    full = shares[0]
    for d in range(1, shares.shape[0]):
        full = full + shares[d]
    full = full / count[...]
    half, total = full.shape[0], full.shape[1] // 2
    cov[:half] = full[:, :total]
    cov[half:] = pltpu.roll(full, total, 1)[:, :total]
    last = pltpu.make_async_copy(cov, cov_out, cov_sem)
    last.start()
    copies.append(last)
    for copy in copies:
        copy.wait()


def solution(mesh):
    n_t, n_s = mesh.shape["tm"], mesh.shape["series"]

    def shards(signal, valid_start, valid_end):
        rows, width = signal.shape
        total = rows * n_s
        quarter = width // n_s
        chunk = chunk_of(quarter)
        per = quarter // chunk
        f32 = jnp.float32
        dma = pltpu.SemaphoreType.DMA
        kept = pl.pallas_call(
            functools.partial(kernel, n_s, n_t, rows, width, chunk),
            out_shape=(
                jax.ShapeDtypeStruct((rows, width), f32),
                jax.ShapeDtypeStruct((rows, width), f32),
                jax.ShapeDtypeStruct((n_t * n_s, rows // 2, 2 * total), f32),
                jax.ShapeDtypeStruct((rows // 2, 2 * total), f32),
            ),
            in_specs=[pl.BlockSpec(memory_space=pltpu.HBM)] * 3,
            out_specs=(pl.BlockSpec(memory_space=pltpu.VMEM),) * 4,
            scratch_shapes=[
                pltpu.SMEM((total,), jnp.int32),
                pltpu.SMEM((total,), jnp.int32),
                pltpu.VMEM((rows, width + 2 * LANE), f32),
                pltpu.VMEM((2 * LANE, 2 * LANE), f32),
                pltpu.VMEM((2, rows, LANE), jnp.int32),
                pltpu.VMEM((rows, width), f32),
                pltpu.VMEM((n_s, rows, quarter), f32),
                pltpu.VMEM((2, rows, LANE), f32),
                pltpu.VMEM((n_s, rows // 2, 2 * total), f32),
                pltpu.VMEM((n_s, rows // 2, 2 * total), f32),
                pltpu.VMEM((2, rows, chunk), f32),
                dma((2,)),
                dma((2,)),
                dma((2,)),
                dma((2,)),
                dma,
                dma((per + 1,)),
                dma((2,)),
                pltpu.SemaphoreType.REGULAR((1 + len(rounds_of(n_t)),)),
                dma((2,)),
                dma((2,)),
            ],
            compiler_params=pltpu.CompilerParams(
                collective_id=0, has_side_effects=True, vmem_limit_bytes=67043328 - 8 * rows * width - 12 * 1024 * 1024
            ),
        )(*[pltpu.with_memory_space_constraint(v, pltpu.HBM) for v in (valid_start, valid_end)], signal)
        return pl.pallas_call(
            flush,
            out_shape=tuple(jax.ShapeDtypeStruct(v, f32) for v in ((rows, width), (rows, width), (rows, total))),
            in_specs=[pl.BlockSpec(memory_space=pltpu.VMEM)] * 4,
            out_specs=(pl.BlockSpec(memory_space=pltpu.HBM),) * 3,
            scratch_shapes=[pltpu.VMEM((rows, total), f32), dma((2 * FLUSHES,)), dma],
            compiler_params=pltpu.CompilerParams(vmem_limit_bytes=1024 * 1024),
        )(*kept)

    in_specs = (P("series", "tm"), P(), P())
    out_specs = (P("series", "tm"), P("series", "tm"), P("series", None))
    return jax.shard_map(shards, mesh=mesh, in_specs=in_specs, out_specs=out_specs, check_vma=False)
```

```python
import functools

import jax
import jax.numpy as jnp
from jax import lax
from jax.experimental import pallas as pl
from jax.experimental.pallas import tpu as pltpu
from jax.sharding import PartitionSpec as P

HALF = 16
LANE = 128
TAPS = 2 * HALF + 1
SECOND = float(sum(j * j for j in range(-HALF, HALF + 1)))
CENTRE_SQ = SECOND / TAPS
FOURTH = float(sum((j * j - CENTRE_SQ) ** 2 for j in range(-HALF, HALF + 1)))
MESH = pl.DeviceIdType.MESH


def chunk_of(quarter):
    chunk = 1024
    while quarter % chunk:
        chunk //= 2
    return chunk


def rounds_of(n_t):
    far = 2 * (2 - n_t % 2)
    rounds = []
    while far < n_t:
        rounds.append(far)
        far *= 2
    return rounds


def kernel(
    n_s, n_t, rows, width, chunk,
    start_hbm, end_hbm, sig_hbm,
    smooth, slope, shares, count,
    starts, stops, ext, wts, ends, res, mixed, halo, part, summed, relay,
    load_sem, bound_sem, halo_send, halo_recv, send_sem, recv_sem, share_sem, met, relay_send, relay_recv,
):
    s = lax.axis_index("series")
    t = lax.axis_index("tm")
    quarter = width // n_s
    per = quarter // chunk
    steps = n_s * per
    sends = (n_s - 1) * per
    total = n_s * rows
    tiles = chunk // LANE
    group = 2 - n_t % 2
    pairs = n_t // group
    rounds = rounds_of(n_t)
    swaps = n_s == 4 and group == 2 and rounds and per >= 8
    f32 = jnp.float32

    def offset(qi):
        if n_s == 4:
            odd = lax.rem(s, 2)
            return jnp.where(qi == 0, 2, jnp.where(qi == 1, 3 - 2 * odd, jnp.where(qi == 2, 1 + 2 * odd, 0)))
        return lax.rem(qi + 1, n_s)

    def fetch(at, size, sem):
        return pltpu.make_async_copy(
            sig_hbm.at[:, pl.ds(pl.multiple_of(at, LANE), size)],
            ext.at[:, pl.ds(pl.multiple_of(at + LANE, LANE), size)],
            load_sem.at[sem])

    head = lax.rem(s + offset(0), n_s) * quarter
    lead = min(chunk + 2 * LANE, quarter - chunk + LANE)
    before = chunk - LANE
    after = quarter - before - lead
    fetch(head + before, lead, 0).start()

    partner = t + 1 - 2 * lax.rem(t, 2)

    def tell(sem, at, ok=None):
        def signal():
            pl.semaphore_signal(sem, inc=1, device_id={"tm": at}, device_id_type=MESH)
        if ok is None:
            signal()
        else:
            pl.when(ok)(signal)

    def reach(sem, far):
        tell(sem, t - far, t >= far)
        tell(sem, t + far, t + far < n_t)

    def heard(far):
        return (t >= far).astype(jnp.int32) + (t + far < n_t).astype(jnp.int32)

    barrier = pltpu.get_barrier_semaphore()
    for d in range(1, n_s):
        pl.semaphore_signal(barrier, inc=1, device_id={"series": lax.rem(s + d, n_s)}, device_id_type=MESH)
    if group == 2:
        tell(barrier, partner)
    reach(barrier, group)

    limits = [
        pltpu.make_async_copy(start_hbm, starts, bound_sem.at[0]),
        pltpu.make_async_copy(end_hbm, stops, bound_sem.at[1]),
    ]
    for limit in limits:
        limit.start()
    fetch(head, before, 1).start()
    if after:
        fetch(head + before + lead, after, 1).start()
    for qi in range(1, n_s):
        fetch(lax.rem(s + offset(qi), n_s) * quarter, quarter, 1).start()

    tap = lax.broadcasted_iota(jnp.int32, (2 * LANE, LANE), 0) - lax.broadcasted_iota(jnp.int32, (2 * LANE, LANE), 1) - HALF
    near = (tap >= -HALF) & (tap <= HALF)
    tap = tap.astype(f32)
    wts[:, :LANE] = jnp.where(near, 1.0 / TAPS - (tap * tap - CENTRE_SQ) * (CENTRE_SQ / FOURTH), 0.0)
    wts[:, LANE:] = jnp.where(near, tap * (HALF / SECOND), 0.0)
    ext[:, :LANE] = jnp.zeros((rows, LANE), f32)
    ext[:, LANE + width :] = jnp.zeros((rows, LANE), f32)

    for limit in limits:
        limit.wait()
    row = lax.broadcasted_iota(jnp.int32, (rows, LANE), 0)
    begin = t * width
    first = jnp.zeros((rows, LANE), jnp.int32)
    last = jnp.zeros((rows, LANE), jnp.int32)
    for i in range(rows):
        first = jnp.where(row == i, starts[s * rows + i], first)
        last = jnp.where(row == i, stops[s * rows + i], last)
    ends[0] = first - begin
    ends[1] = last - begin

    def held(v, base):
        lanes = lax.broadcasted_iota(jnp.int32, (rows, LANE), 1)
        found = []
        for spot in (ends[0] + LANE - base, ends[1] - TAPS + LANE - base):
            tile = lax.shift_right_arithmetic(spot, LANE.bit_length() - 1)
            pair = [jnp.zeros((rows, LANE), f32)] * 2
            for n in range(tiles + 1):
                here = tile == n
                for w in range(2):
                    pair[w] = jnp.where(here, v[:, (n + w) * LANE : (n + w + 1) * LANE], pair[w])
            j = lanes - (spot - tile * LANE + HALF)
            sums = []
            for j, win in ((j, pair[0]), (j + LANE, pair[1])):
                win = jnp.where((j >= -HALF) & (j <= HALF), win, 0.0)
                j = j.astype(f32)
                sums.append((win, win * j, win * (j * j - CENTRE_SQ)))
            for m, scale in enumerate((1.0 / TAPS, 1.0 / SECOND, 1.0 / FOURTH)):
                value = jnp.sum(sums[0][m] + sums[1][m], axis=1, keepdims=True) * scale
                found.append(jnp.broadcast_to(value, (rows, LANE)))
        return found

    right, left = lax.rem(t + 1, n_t), lax.rem(t + n_t - 1, n_t)
    to_right = pltpu.make_async_remote_copy(
        ext.at[:, pl.ds(width, LANE)], halo.at[0], halo_send.at[0], halo_recv.at[0],
        device_id={"tm": right}, device_id_type=MESH)
    to_left = pltpu.make_async_remote_copy(
        ext.at[:, pl.ds(LANE, LANE)], halo.at[1], halo_send.at[1], halo_recv.at[1],
        device_id={"tm": left}, device_id_type=MESH)
    has_right, has_left = t < n_t - 1, t > 0

    mirror = t + group * (pairs - 1 - 2 * lax.div(t, group))
    gap = lax.div(t - mirror, group)
    whole_from, whole_to = gap == 3, gap == -3
    half_from, half_to = gap == 1, gap == -1
    side_from, side_to = lax.rem(t, 2) == 1, lax.rem(t, 2) == 0
    detour = per + 2
    lag = per
    slip = 3 * chunk // 8
    across = lax.rem(s + offset(1), n_s)

    def place(k):
        qi = k // per
        q = lax.rem(s + offset(qi), n_s)
        j = lax.rem(lax.rem(k, per) + 1, per)
        return q, j

    def transfer(k):
        q, j = place(k)
        return pltpu.make_async_remote_copy(
            res.at[:, pl.ds(pl.multiple_of(q * quarter + j * chunk, chunk), chunk)],
            mixed.at[s, :, pl.ds(pl.multiple_of(j * chunk, chunk), chunk)],
            send_sem, recv_sem.at[(j + 1) // 2 if isinstance(j, int) else lax.div(j + 1, 2)],
            device_id={"series": q}, device_id_type=MESH)

    def column(j):
        return pl.multiple_of(j * chunk, chunk)

    tail = chunk // 4

    def closing(k, at, size, sem):
        q, j = place(k)
        return pltpu.make_async_remote_copy(
            res.at[:, pl.ds(column(q * per + j) + at, size)], mixed.at[s, :, pl.ds(column(j) + at, size)],
            send_sem, recv_sem.at[sem],
            device_id={"series": q}, device_id_type=MESH)

    def send(k):
        ends_here = lax.rem(k, per) == per - 1

        @pl.when(jnp.logical_not(ends_here))
        def _():
            transfer(k).start()

        @pl.when(ends_here)
        def _():
            closing(k, 0, chunk - tail, 0).start()
            closing(k, chunk - tail, tail, per // 2 + 1).start()

    def away(k, n):
        q, j = place(k)
        size = chunk if n == 0 else chunk // 4
        return pltpu.make_async_remote_copy(
            res.at[:, pl.ds(column(q * per + j), size)], relay.at[0, :, pl.ds(0, size)],
            send_sem, relay_recv.at[0],
            device_id={"series": across, "tm": mirror}, device_id_type=MESH)

    def onward(n):
        j = detour + n - per + 1
        size = chunk if n == 0 else chunk // 4
        return pltpu.make_async_remote_copy(
            relay.at[0, :, pl.ds(0, size)], mixed.at[across, :, pl.ds(j * chunk, size)],
            relay_send.at[0], recv_sem.at[(j + 1) // 2 if isinstance(j, int) else lax.div(j + 1, 2)],
            device_id={"tm": mirror}, device_id_type=MESH)

    def aside():
        q, j = place(detour - 1)
        return pltpu.make_async_remote_copy(
            res.at[:, pl.ds(column(q * per + j), slip)], relay.at[1, :, pl.ds(0, slip)],
            send_sem, relay_recv.at[1],
            device_id={"tm": partner}, device_id_type=MESH)

    def over():
        j = detour - per
        return pltpu.make_async_remote_copy(
            relay.at[1, :, pl.ds(0, slip)], mixed.at[s, :, pl.ds(j * chunk, slip)],
            relay_send.at[1], recv_sem.at[(j + 1) // 2 if isinstance(j, int) else lax.div(j + 1, 2)],
            device_id={"series": across, "tm": partner}, device_id_type=MESH)

    def rest(k, at):
        q, j = place(k)
        return pltpu.make_async_remote_copy(
            res.at[:, pl.ds(column(q * per + j) + at, chunk - at)],
            mixed.at[s, :, pl.ds(column(j) + at, chunk - at)],
            send_sem, recv_sem.at[(j + 1) // 2 if isinstance(j, int) else lax.div(j + 1, 2)],
            device_id={"series": q}, device_id_type=MESH)

    def greeting(i):
        if 0 < i <= len(rounds):
            pl.semaphore_wait(met.at[i], heard(rounds[i - 1]))
        if i < len(rounds):
            reach(met.at[i + 1], rounds[i])

    def spread(v):
        return jnp.concatenate([v] * tiles, axis=1)

    greet = min(3, per - 3)

    def step(k, carry):
        @pl.when(k == 0)
        def _():
            fetch(0, lead, 0).wait()

        @pl.when(k == 1)
        def _():
            fetch(0, width - lead, 1).wait()

        @pl.when(k == per - 2)
        def _():
            @pl.when(has_left)
            def _():
                to_right.wait_recv()
                ext[:, :LANE] = halo[0]

            @pl.when(has_right)
            def _():
                to_left.wait_recv()
                ext[:, LANE + width :] = halo[1]

        q, j = place(k)
        base = pl.multiple_of(q * quarter + j * chunk, chunk)
        v = ext[:, pl.ds(base, chunk + 2 * LANE)]
        moved = pltpu.roll(v, chunk + LANE + HALF, 1)
        lines = jnp.concatenate([moved[:, n * LANE : (n + 2) * LANE] for n in range(tiles)], axis=0)
        out = jnp.dot(lines, wts[...], precision=lax.Precision.HIGHEST, preferred_element_type=f32)
        sm = jnp.concatenate([out[n * rows : (n + 1) * rows, :LANE] for n in range(tiles)], axis=1)
        sl = jnp.concatenate([out[n * rows : (n + 1) * rows, LANE:] for n in range(tiles)], axis=1)
        moment = base + lax.broadcasted_iota(jnp.int32, (rows, chunk), 1)
        low = moment - spread(ends[0])
        high = moment - spread(ends[1])
        coef = held(v, base)
        inside = (low >= 0) & (high < 0)
        below = low < HALF
        above = high >= -HALF
        along = jnp.where(below, low - HALF, high + HALF + 1).astype(f32)
        lv = jnp.where(below, spread(coef[0]), spread(coef[3]))
        tl = jnp.where(below, spread(coef[1]), spread(coef[4]))
        bd = jnp.where(below, spread(coef[2]), spread(coef[5]))
        end = below | above
        sm = jnp.where(end, lv + tl * along + bd * (along * along - CENTRE_SQ), sm)
        sl = jnp.where(end, HALF * (tl + 2.0 * along * bd), sl)
        sm = jnp.where(inside, sm, 0.0)
        smooth[:, pl.ds(base, chunk)] = sm
        slope[:, pl.ds(base, chunk)] = jnp.where(inside, sl, 0.0)
        rs = jnp.where(inside, v[:, LANE : LANE + chunk] - sm, 0.0)

        @pl.when(k < sends)
        def _():
            res[:, pl.ds(base, chunk)] = rs

        @pl.when(k >= sends)
        def _():
            mixed[s, :, pl.ds(pl.multiple_of(j * chunk, chunk), chunk)] = rs

        @pl.when(k == 0)
        def _():
            pl.semaphore_wait(barrier, n_s - 1 + group - 1 + heard(group))
            if group == 2:
                tell(met.at[0], partner)
            reach(met.at[0], group)

        @pl.when(k == greet)
        def _():
            pl.semaphore_wait(met.at[0], group - 1 + heard(group))

            @pl.when(has_right)
            def _():
                to_right.start()

            @pl.when(has_left)
            def _():
                to_left.start()

            greeting(0)

        @pl.when(k == max(detour, greet + 1))
        def _():
            greeting(1)

        if not swaps:
            @pl.when(k < sends)
            def _():
                send(k)

            return carry

        @pl.when((k == detour - 1) & side_from)
        def _():
            aside().start()

        @pl.when((k == detour) & whole_from)
        def _():
            away(k, 0).start()

        @pl.when((k == detour + 1) & half_from)
        def _():
            away(k, 1).start()

        @pl.when((k == per + lag) & side_to)
        def _():
            aside().wait_recv()
            over().start()

        m = jnp.where(k < per, k, k - lag)
        fork, split = (m == detour - 1) & side_from, (m == detour + 1) & half_from
        ready = (k < per) | ((k >= per + lag) & (m < sends))

        @pl.when(ready & jnp.logical_not(fork | split | ((m == detour) & whole_from)))
        def _():
            send(m)

        @pl.when(ready & fork)
        def _():
            rest(m, slip).start()

        @pl.when(ready & split)
        def _():
            rest(m, chunk // 4).start()

        return carry

    lax.fori_loop(0, steps, step, 0)

    def pass_on(n):
        def move():
            away(detour + n, n).wait_recv()
            onward(n).start()
        return move

    if swaps:
        for m in range(steps - lag, sends):
            send(m)
        pl.when(whole_to)(pass_on(0))
        pl.when(half_to)(pass_on(1))

    def arrival(at, size, sem):
        block = mixed.at[pl.ds(0, n_s - 1), :, pl.ds(at, size)]
        return pltpu.make_async_remote_copy(
            block, block, send_sem, recv_sem.at[sem],
            device_id={"series": lax.rem(s + 1, n_s)}, device_id_type=MESH)

    half = rows // 2
    left_half = lax.broadcasted_iota(jnp.int32, (half, 2 * total), 1) < total

    def pack(v):
        return jnp.where(left_half, v[:half], v[half:])

    gram = jnp.zeros((2 * total, 2 * total), f32)
    parts = [(j * chunk, min(2, per - j) * chunk, (j + 1) // 2) for j in range(1, per, 2)]
    parts += [(0, chunk - tail, 0), (chunk - tail, tail, per // 2 + 1)]
    for i, (at, size, sem) in enumerate(parts):
        greeting(i + 2)
        arrival(at, size, sem).wait_recv()
        x = jnp.concatenate([mixed[g, :, at : at + size] for g in range(n_s)], axis=0)
        hi = x.astype(jnp.bfloat16)
        lo = (x - hi.astype(f32)).astype(jnp.bfloat16)
        z = jnp.concatenate([hi, lo], axis=0)
        gram = gram + lax.dot_general(z, z, (((1,), (1,)), ((), ())), preferred_element_type=f32)
    for i in range(len(parts) + 2, len(rounds) + 1):
        greeting(i)
    both = gram[:total] + gram[total:]
    both = both + pltpu.roll(both, total, 1)
    here = t * n_s + s
    whole = n_t * n_s
    nest = n_t * n_s // 2
    first_in = (t == 0) & (s < 2)

    def early(to_s):
        return pltpu.make_async_remote_copy(
            part.at[to_s], shares.at[here], share_sem.at[0], share_sem.at[1],
            device_id={"tm": 0, "series": to_s}, device_id_type=MESH)

    for g in range(n_s):
        part[g] = pack(both[g * rows : (g + 1) * rows])
    for g in range(2):
        @pl.when((t != 0) | (s != g))
        def _():
            early(g).start()


    core = lax.rem(s, 2)
    mate = s + 1 - 2 * core

    def swap(g):
        return pltpu.make_async_remote_copy(
            part.at[g * 2 + 1 - core], summed.at[n_s // 2 + g], load_sem.at[0], load_sem.at[1],
            device_id={"series": mate}, device_id_type=MESH)

    for g in range(n_s // 2):
        swap(g).start()
    got = summed.at[pl.ds(n_s // 2, n_s // 2)]
    both_swaps = pltpu.make_async_remote_copy(
        got, got, load_sem.at[0], load_sem.at[1], device_id={"series": mate}, device_id_type=MESH)
    both_swaps.wait_recv()
    for g in range(n_s // 2):
        summed[g] = part[g * 2 + core] + summed[n_s // 2 + g]

    def share(to_t, to_x):
        return pltpu.make_async_remote_copy(
            summed.at[to_x], shares.at[t * (n_s // 2) + lax.div(s, 2)], share_sem.at[0], share_sem.at[1],
            device_id={"tm": to_t, "series": to_x * 2 + core}, device_id_type=MESH)

    def spread_shares(i, carry):
        beyond = i - group
        beyond = (1 + lax.rem(beyond, pairs - 1)) * group + lax.div(beyond, pairs - 1)
        to_t = jnp.where(i < group, i, beyond)
        for to_x in range(n_s // 2):
            @pl.when(((to_t != t) | (lax.div(s, 2) != to_x)) & ((to_t != 0) | (to_x != 0)))
            def _():
                share(to_t, to_x).start()

        return carry

    lax.fori_loop(0, n_t, spread_shares, 0)
    both_swaps.wait_send()

    @pl.when(first_in)
    def _():
        shares[here] = part[s]

    @pl.when(jnp.logical_not(first_in))
    def _():
        shares[t * (n_s // 2) + lax.div(s, 2)] = summed[lax.div(s, 2)]
        shares[nest:] = jnp.zeros((whole - nest, half, 2 * total), f32)

    lane = lax.broadcasted_iota(jnp.int32, (rows, 2 * total), 1)
    lane = jnp.where(lane < total, lane, lane - total)
    first_k = jnp.zeros((rows, 2 * total), jnp.int32)
    last_k = jnp.zeros((rows, 2 * total), jnp.int32)
    for i in range(total):
        first_k = jnp.where(lane == i, starts[i], first_k)
        last_k = jnp.where(lane == i, stops[i], last_k)
    count[...] = pack((jnp.minimum(last_k, last) - jnp.maximum(first_k, first)).astype(f32))

    sent = res.at[:, pl.ds(0, sends * chunk)]
    pltpu.make_async_remote_copy(
        sent, sent, send_sem, recv_sem.at[0],
        device_id={"series": lax.rem(s + 1, n_s)}, device_id_type=MESH).wait_send()

    @pl.when(has_right)
    def _():
        to_right.wait_send()

    @pl.when(has_left)
    def _():
        to_left.wait_send()

    if swaps:
        pl.when(whole_to)(onward(0).wait_send)
        pl.when(half_to)(onward(1).wait_send)
        pl.when(side_to)(over().wait_send)
    def batch(n):
        block = shares.at[pl.ds(0, n)]
        return pltpu.make_async_remote_copy(
            block, block, share_sem.at[0], share_sem.at[1],
            device_id={"series": lax.rem(s + 1, n_s)}, device_id_type=MESH)

    pl.when(first_in)(batch(whole - 1).wait_recv)
    pl.when(jnp.logical_not(first_in))(batch(nest - 1).wait_recv)
    batch(nest).wait_send()


FLUSHES = 1


def flush(smooth, slope, shares, count, smooth_out, slope_out, cov_out, cov, sems, cov_sem):
    piece = smooth.shape[1] // FLUSHES
    copies = []
    for i in range(FLUSHES):
        span = pl.ds(i * piece, piece)
        copies.append(pltpu.make_async_copy(smooth.at[:, span], smooth_out.at[:, span], sems.at[2 * i]))
        copies.append(pltpu.make_async_copy(slope.at[:, span], slope_out.at[:, span], sems.at[2 * i + 1]))
    for copy in copies:
        copy.start()
    full = shares[0]
    for d in range(1, shares.shape[0]):
        full = full + shares[d]
    full = full / count[...]
    half, total = full.shape[0], full.shape[1] // 2
    cov[:half] = full[:, :total]
    cov[half:] = pltpu.roll(full, total, 1)[:, :total]
    last = pltpu.make_async_copy(cov, cov_out, cov_sem)
    last.start()
    copies.append(last)
    for copy in copies:
        copy.wait()


def solution(mesh):
    n_t, n_s = mesh.shape["tm"], mesh.shape["series"]

    def shards(signal, valid_start, valid_end):
        rows, width = signal.shape
        total = rows * n_s
        quarter = width // n_s
        chunk = chunk_of(quarter)
        per = quarter // chunk
        f32 = jnp.float32
        dma = pltpu.SemaphoreType.DMA
        kept = pl.pallas_call(
            functools.partial(kernel, n_s, n_t, rows, width, chunk),
            out_shape=(
                jax.ShapeDtypeStruct((rows, width), f32),
                jax.ShapeDtypeStruct((rows, width), f32),
                jax.ShapeDtypeStruct((n_t * n_s, rows // 2, 2 * total), f32),
                jax.ShapeDtypeStruct((rows // 2, 2 * total), f32),
            ),
            in_specs=[pl.BlockSpec(memory_space=pltpu.HBM)] * 3,
            out_specs=(pl.BlockSpec(memory_space=pltpu.VMEM),) * 4,
            scratch_shapes=[
                pltpu.SMEM((total,), jnp.int32),
                pltpu.SMEM((total,), jnp.int32),
                pltpu.VMEM((rows, width + 2 * LANE), f32),
                pltpu.VMEM((2 * LANE, 2 * LANE), f32),
                pltpu.VMEM((2, rows, LANE), jnp.int32),
                pltpu.VMEM((rows, width), f32),
                pltpu.VMEM((n_s, rows, quarter), f32),
                pltpu.VMEM((2, rows, LANE), f32),
                pltpu.VMEM((n_s, rows // 2, 2 * total), f32),
                pltpu.VMEM((n_s, rows // 2, 2 * total), f32),
                pltpu.VMEM((2, rows, chunk), f32),
                dma((2,)),
                dma((2,)),
                dma((2,)),
                dma((2,)),
                dma,
                dma((per // 2 + 2,)),
                dma((2,)),
                pltpu.SemaphoreType.REGULAR((1 + len(rounds_of(n_t)),)),
                dma((2,)),
                dma((2,)),
            ],
            compiler_params=pltpu.CompilerParams(
                collective_id=0, has_side_effects=True, vmem_limit_bytes=67043328 - 8 * rows * width - 12 * 1024 * 1024
            ),
        )(*[pltpu.with_memory_space_constraint(v, pltpu.HBM) for v in (valid_start, valid_end)], signal)
        return pl.pallas_call(
            flush,
            out_shape=tuple(jax.ShapeDtypeStruct(v, f32) for v in ((rows, width), (rows, width), (rows, total))),
            in_specs=[pl.BlockSpec(memory_space=pltpu.VMEM)] * 4,
            out_specs=(pl.BlockSpec(memory_space=pltpu.HBM),) * 3,
            scratch_shapes=[pltpu.VMEM((rows, total), f32), dma((2 * FLUSHES,)), dma],
            compiler_params=pltpu.CompilerParams(vmem_limit_bytes=1024 * 1024),
        )(*kept)

    in_specs = (P("series", "tm"), P(), P())
    out_specs = (P("series", "tm"), P("series", "tm"), P("series", None))
    return jax.shard_map(shards, mesh=mesh, in_specs=in_specs, out_specs=out_specs, check_vma=False)
```
